32 devices in a mesh: rows: 8 (over z, x), half: 4 (over y, core).
Axes of the slice: x: 2, y: 2, z: 4, core: 2. Of those that a mesh axis runs over, the one named last changes fastest.
Arguments:
- micrograph: bfloat16 [4096, 4096], P('rows', 'half'), may hold values from -6 to 6
- box_tops: int32 [8, 4, 4, 2], replicated, may hold values from 0 to 3840, as said below
- box_live: int32 [8, 4, 4], replicated, may hold values from 0 to 1, as said below
- box_class: int32 [8, 4, 4], replicated, may hold values from 0 to 49
- box_shift: int32 [8, 4, 4, 2], P('rows', 'half'), may hold values from -8 to 8
Outputs:
- power: float32 [4, 1024, 4096], P('half', 'rows')
- class_means: float32 [50, 2, 256, 256], P(None, None, 'rows', 'half')
The draws below stay inside these ranges and needn't reach their ends.
Inputs may be any that keep to these rules, and one draw needn't show every extreme that they name: `box_tops`: the box of every slot lies inside the micrograph. A slot of box_live = 1 at index (i, j, s) has its first row among rows i * 512 to (i + 1) * 512 - 1. `box_live`: in each device's slots the live ones come first; in every draw some device has all 4 slots live.
All inputs are finite; a program needn't handle non-finite values.
Results may differ from the reference program's by a relative error of at most 0.0029.
Values may be sent and summed in bfloat16 or wider, within the bound.
No kernel may reach another device: no remote copies, remote signals or barrier semaphores. Data moves between devices by JAX's collectives and lax.ppermute only.
A program may use at most 64 MiB of HBM per device.

```python
import jax
import jax.numpy as jnp
from jax import lax

NPIX = 4096
BOX = 256
CLASSES = 50
CAP = 4
SHIFT = 8
BANDS = 8
QUARTERS = 4
N_HALF = 4


def draw_box_tops(key, part):
    base_key = jax.random.fold_in(key, 17)
    key_rows, key_cols = jax.random.split(base_key)
    band_rows = NPIX // BANDS
    within = jax.random.randint(key_rows, (BANDS, QUARTERS, CAP), 0, band_rows)
    starts = jnp.arange(BANDS, dtype=jnp.int32)[:, None, None] * band_rows + within
    starts = jnp.minimum(starts, NPIX - BOX)
    columns = jax.random.randint(key_cols, (BANDS, QUARTERS, CAP), 0, NPIX - BOX + 1)
    return jnp.stack([starts, columns], axis=-1).astype(jnp.int32)


def draw_box_live(key, part):
    base_key = jax.random.fold_in(key, 31)
    key_one, key_three = jax.random.split(base_key, 2)
    missing = jax.random.randint(key_one, (BANDS, QUARTERS), 0, max(CAP // 2, 1) + 1)
    counts = CAP - missing
    usable = (NPIX - BOX) // (NPIX // BANDS) + 1
    chosen = jax.random.randint(key_three, (), 0, usable * QUARTERS)
    flat_index = jnp.arange(BANDS * QUARTERS, dtype=jnp.int32).reshape(BANDS, QUARTERS)
    counts = jnp.where(flat_index == chosen, CAP, counts)
    band_index = flat_index // QUARTERS
    counts = jnp.where(band_index < usable, counts, 0)
    slot_index = jnp.arange(CAP, dtype=jnp.int32)
    return (slot_index[None, None, :] < counts[:, :, None]).astype(jnp.int32)


def set_ends(array, own_key, smallest, top_value):
    longest = array.shape.index(max(array.shape))
    spots = []
    for shift in (0, 1):
        where = [jax.random.randint(jax.random.fold_in(own_key, axis), (), 0, length) for axis, length in enumerate(array.shape)]
        where[longest] = (where[longest] + shift) % array.shape[longest]
        spots.append(tuple(where))
    return array.at[spots[0]].set(smallest).at[spots[1]].set(top_value)


def levels(own_key, extent, cuts, low, top_value):
    gain, own = 1.0, jax.random.fold_in(own_key, 6)
    for axis_at, shards_of in cuts:
        steps = jnp.exp(jax.random.uniform(jax.random.fold_in(own, axis_at), (shards_of,), jnp.float32, low / len(cuts), top_value / len(cuts)))
        gain = gain * jnp.repeat(steps, extent[axis_at] // shards_of).reshape([-1 if axis == axis_at else 1 for axis in range(len(extent))])
    return gain


def normal_values(own_key, dims, width, reach, cuts=(), kind=jnp.bfloat16):
    array = jax.random.normal(own_key, dims, jnp.float32) * width
    if len(cuts) > 0:
        array = levels(own_key, dims, cuts, -0.22, 0.18) * array
    return jnp.clip(array, min=-reach, max=reach).astype(kind)


def setup_inputs(seed: int = 0) -> dict:
    streams_of = jax.random.split(jax.random.key(seed), 6)
    micrograph = normal_values(streams_of[0], (NPIX, NPIX), 1.0, 6.0, ((0, 8), (1, 4)))
    box_tops = draw_box_tops(jax.random.fold_in(streams_of[5], 71), 0)
    box_live = draw_box_live(jax.random.fold_in(streams_of[5], 71), 0)
    box_class = set_ends(jax.random.randint(streams_of[3], (BANDS, QUARTERS, CAP), 0, CLASSES), jax.random.fold_in(streams_of[3], 1), 0, CLASSES - 1).astype(jnp.int32)
    box_shift = set_ends(jax.random.randint(streams_of[4], (BANDS, QUARTERS, CAP, 2), -SHIFT, SHIFT + 1), jax.random.fold_in(streams_of[4], 1), -SHIFT, SHIFT).astype(jnp.int32)
    return dict(micrograph=micrograph, box_tops=box_tops, box_live=box_live, box_class=box_class, box_shift=box_shift)


def reference(micrograph, box_tops, box_live, box_class, box_shift):
    image_rows = micrograph.astype(jnp.float32)
    spectrum = jnp.fft.fft2(image_rows)
    real_part = jnp.real(spectrum)
    imag_part = jnp.imag(spectrum)
    power_out = (real_part * real_part + imag_part * imag_part) / (NPIX * NPIX)
    power_out = power_out.T.reshape(N_HALF, NPIX // N_HALF, NPIX)

    tops_flat = box_tops.reshape(-1, 2).astype(jnp.int32)
    shifts_flat = box_shift.reshape(-1, 2).astype(jnp.int32)
    live_flat = box_live.reshape(-1)
    labels = box_class.reshape(-1).astype(jnp.int32)
    frequency = jnp.arange(BOX, dtype=jnp.int32)

    def accumulate(totals, member):
        corner, offsets_pair, weight, label = member
        particle = lax.dynamic_slice(image_rows, (corner[0], corner[1]), (BOX, BOX))
        transformed = jnp.fft.fft2(particle) / BOX
        rotations = jnp.mod(frequency[:, None] * offsets_pair[0] + frequency[None, :] * offsets_pair[1], BOX)
        angles = (2.0 * jnp.pi / BOX) * rotations.astype(jnp.float32)
        ramp_cos = jnp.cos(angles)
        ramp_sin = jnp.sin(angles)
        trans_real = jnp.real(transformed)
        trans_imag = jnp.imag(transformed)
        out_real = trans_real * ramp_cos + trans_imag * ramp_sin
        out_imag = trans_imag * ramp_cos - trans_real * ramp_sin
        paired = jnp.stack([out_real, out_imag]).astype(jnp.bfloat16)
        paired = lax.optimization_barrier(paired).astype(jnp.float32)
        totals = totals.at[label].add(weight.astype(jnp.float32) * paired)
        return totals, None

    empty = jnp.zeros((CLASSES, 2, BOX, BOX), jnp.float32)
    totals, unused = lax.scan(accumulate, empty, (tops_flat, shifts_flat, live_flat, labels))
    classes_all = jnp.arange(CLASSES, dtype=jnp.int32)
    counts = jnp.sum((labels[None, :] == classes_all[:, None]).astype(jnp.int32) * live_flat[None, :], axis=1)
    divisor = jnp.maximum(counts, 1).astype(jnp.float32)
    class_means = totals / divisor[:, None, None, None]
    return power_out, class_means
```

```python
import functools

import numpy as np

import jax
import jax.numpy as jnp
from jax import lax
from jax.experimental import pallas as pl
from jax.experimental.pallas import tpu as pltpu
from jax.sharding import PartitionSpec as P

BOX = 256
CLASSES = 50
RADIX = 64
LANES = 128
POINTS = 16

highest = lax.Precision.HIGHEST


def passed_along(block, axis, distance):
    devices = range(lax.axis_size(axis))
    route = [(i - distance, i) for i in devices if i - distance in devices]
    return lax.ppermute(block, axis, route)


def phases(left_index, right_index, length):
    rotations = jnp.mod(left_index[:, None] * right_index[None, :], length)
    angles = 2.0 * jnp.pi / length * rotations.astype(jnp.float32)
    return (jnp.cos(angles), jnp.sin(angles))


def product(pattern, left_side, matrix):
    return jnp.einsum(pattern, left_side, matrix, precision=highest)


def four_step(real_part, imag_part, first_index, how_many, rows_last):
    height = real_part.shape[0]
    length = real_part.shape[1]
    outer_size = RADIX
    inner_size = length // outer_size
    real_part = real_part.reshape(height, outer_size, inner_size)
    spread = jnp.arange(outer_size, dtype=jnp.int32)
    across = jnp.arange(inner_size, dtype=jnp.int32)
    cos_one, sin_one = phases(spread, spread, outer_size)
    section_real = product("mab,ka->mkb", real_part, cos_one)
    section_imag = -product("mab,ka->mkb", real_part, sin_one)
    if imag_part is not None:
        imag_part = imag_part.reshape(height, outer_size, inner_size)
        section_real = section_real + product("mab,ka->mkb", imag_part, sin_one)
        section_imag = section_imag + product("mab,ka->mkb", imag_part, cos_one)
    twist_cos, twist_sin = phases(spread, across, length)
    turned_real = section_real * twist_cos + section_imag * twist_sin
    turned_imag = section_imag * twist_cos - section_real * twist_sin
    wanted = first_index + jnp.arange(how_many, dtype=jnp.int32)
    cos_two, sin_two = phases(wanted, across, inner_size)
    pattern = "mkb,tb->tkm" if rows_last else "mkb,tb->mtk"
    out_real = product(pattern, turned_real, cos_two) + product(pattern, turned_imag, sin_two)
    out_imag = product(pattern, turned_imag, cos_two) - product(pattern, turned_real, sin_two)
    return (out_real, out_imag)


def general_device(micrograph, box_tops, box_live, box_class, box_shift):
    row_index = lax.axis_index("rows")
    half_index = lax.axis_index("half")
    band_rows = lax.all_gather(micrograph, "half", axis=1, tiled=True)
    height = band_rows.shape[0]
    full_width = band_rows.shape[1]
    quarter = full_width // lax.axis_size("half")
    per_block = quarter // RADIX
    image_rows = band_rows.astype(jnp.float32)
    part_real, part_imag = four_step(image_rows, None, half_index * per_block, per_block, True)
    partial_value = jnp.stack(
        [part_real.reshape(quarter, height), part_imag.reshape(quarter, height)]
    )
    columns = lax.all_to_all(partial_value, "rows", split_axis=1, concat_axis=2, tiled=True)
    column_count = columns.shape[1]
    freq_real, freq_imag = four_step(columns[0], columns[1], 0, full_width // RADIX, False)
    power_out = (freq_real * freq_real + freq_imag * freq_imag).reshape(1, column_count, full_width)
    power_out = power_out / (full_width * full_width)
    local_tops = box_tops[row_index, half_index]
    start_rows = local_tops[:, 0] - row_index * height
    start_cols = local_tops[:, 1]
    reach_bands = (BOX + height - 2) // height

    def cut_columns(source, corner):
        return lax.dynamic_slice_in_dim(source, corner, BOX, 1)

    pieces = [jax.vmap(cut_columns, (None, 0))(band_rows, start_cols)]
    for offset in range(1, reach_bands + 1):
        target = jnp.maximum(row_index - offset, 0)
        their_cols = box_tops[target, half_index][:, 1]
        outgoing = jax.vmap(cut_columns, (None, 0))(band_rows, their_cols)
        pieces.append(passed_along(outgoing, "rows", -offset))
    windows = jnp.concatenate(pieces, axis=1)
    particle_boxes = jax.vmap(
        lambda window, corner: lax.dynamic_slice_in_dim(window, corner, BOX, 0)
    )(windows, start_rows)
    frequency = jnp.arange(BOX, dtype=jnp.int32)
    cos_box, sin_box = phases(frequency, frequency, BOX)
    local_offsets = box_shift.reshape(-1, 2)

    def spectrum(member):
        particle, offsets_pair = member
        values = particle.astype(jnp.float32)
        inner_real = jnp.dot(values, cos_box, precision=highest)
        inner_imag = -jnp.dot(values, sin_box, precision=highest)
        outer_real = (
            jnp.dot(cos_box, inner_real, precision=highest)
            + jnp.dot(sin_box, inner_imag, precision=highest)
        ) / BOX
        outer_imag = (
            jnp.dot(cos_box, inner_imag, precision=highest)
            - jnp.dot(sin_box, inner_real, precision=highest)
        ) / BOX
        rotations = jnp.mod(
            frequency[:, None] * offsets_pair[0] + frequency[None, :] * offsets_pair[1], BOX
        )
        angles = 2.0 * jnp.pi / BOX * rotations.astype(jnp.float32)
        ramp_cos = jnp.cos(angles)
        ramp_sin = jnp.sin(angles)
        shifted_real = outer_real * ramp_cos + outer_imag * ramp_sin
        shifted_imag = outer_imag * ramp_cos - outer_real * ramp_sin
        return jnp.stack([shifted_real, shifted_imag]).astype(jnp.bfloat16)

    spectra = lax.map(spectrum, (particle_boxes, local_offsets))
    classes_all = jnp.arange(CLASSES, dtype=jnp.int32)
    all_labels = box_class.reshape(-1)
    all_live = box_live.reshape(-1)
    counts = jnp.sum(
        (all_labels[None, :] == classes_all[:, None]).astype(jnp.int32) * all_live[None, :], axis=1
    )
    arrived = lax.all_to_all(spectra, "rows", split_axis=2, concat_axis=0, tiled=True)
    chosen_labels = box_class[:, half_index].reshape(-1)
    chosen_live = box_live[:, half_index].reshape(-1)
    weights = (
        (chosen_labels[None, :] == classes_all[:, None]).astype(jnp.int32) * chosen_live[None, :]
    ).astype(jnp.bfloat16)
    flat_spectra = arrived.reshape(arrived.shape[0], -1)
    partial_sums = jnp.dot(weights, flat_spectra, preferred_element_type=jnp.float32)
    partial_sums = partial_sums.reshape((CLASSES,) + arrived.shape[1:])
    class_sums = lax.psum_scatter(partial_sums, "half", scatter_dimension=3, tiled=True)
    divisor = jnp.maximum(counts, 1).astype(jnp.float32)
    class_means = class_sums / divisor[:, None, None, None]
    return (power_out, class_means)


f32 = jnp.float32
bf16 = jnp.bfloat16
VMEM = pl.BlockSpec(memory_space=pltpu.VMEM)
SMEM = pl.BlockSpec(memory_space=pltpu.SMEM)


def call(kernel, out, operands, specs, scratch=(), flops=0):
    moved = sum(a.size * a.dtype.itemsize for a in operands) + out.size * out.dtype.itemsize
    return pl.pallas_call(
        kernel,
        out_shape=out,
        in_specs=specs,
        out_specs=VMEM,
        scratch_shapes=list(scratch),
        compiler_params=pltpu.CompilerParams(vmem_limit_bytes=48 * 1024 * 1024),
        cost_estimate=pl.CostEstimate(flops=flops, bytes_accessed=moved, transcendentals=0),
    )(*operands)


def halves(table):
    high = table.astype(bf16)
    low = (table - high.astype(np.float64)).astype(bf16)
    return high, low


def waves(left, right, length):
    angles = 2.0 * np.pi / length * np.mod(np.outer(left, right), length)
    return np.cos(angles), np.sin(angles)


def dft4(re, im):
    sr, si = re[0] + re[2], im[0] + im[2]
    dr, di = re[0] - re[2], im[0] - im[2]
    tr, ti = re[1] + re[3], im[1] + im[3]
    er, ei = re[1] - re[3], im[1] - im[3]
    return [sr + tr, dr + ei, sr - tr, dr - ei], [si + ti, di - er, si - ti, di + er]


def turn(re, im, step):
    step = step % POINTS
    if step == 0:
        return re, im
    if step == POINTS // 4:
        return im, -re
    c = float(np.cos(2.0 * np.pi * step / POINTS))
    s = float(np.sin(2.0 * np.pi * step / POINTS))
    if step == POINTS // 8:
        return (re + im) * c, (im - re) * c
    if step == 3 * POINTS // 8:
        return (im - re) * s, (re + im) * -s
    return re * c + im * s, im * c - re * s


def dft16(re, im):
    mid_re = [[None] * 4 for _ in range(4)]
    mid_im = [[None] * 4 for _ in range(4)]
    for n in range(4):
        yr, yi = dft4([re[4 * p + n] for p in range(4)], [im[4 * p + n] for p in range(4)])
        for k in range(4):
            mid_re[k][n], mid_im[k][n] = turn(yr[k], yi[k], n * k)
    out_re, out_im = [None] * POINTS, [None] * POINTS
    for k in range(4):
        yr, yi = dft4(mid_re[k], mid_im[k])
        for m in range(4):
            out_re[k + 4 * m], out_im[k + 4 * m] = yr[m], yi[m]
    return out_re, out_im


def dot(a, b):
    return jnp.dot(a, b, preferred_element_type=f32)


def prepare_kernel(n_half, x_ref, y_ref):
    height, quarter = x_ref.shape
    rows_each = height // POINTS
    kept = POINTS // n_half
    cols_each = quarter // POINTS
    share = height // n_half
    place = lax.broadcasted_iota(jnp.int32, (height, height), 0)
    source = lax.broadcasted_iota(jnp.int32, (height, height), 1)
    wanted = (place % rows_each) * POINTS + place // rows_each
    pick_rows = jnp.where(source == wanted, 1.0, 0.0).astype(bf16)
    ordered = dot(pick_rows, x_ref[...]).astype(bf16)
    place = lax.broadcasted_iota(jnp.int32, (quarter, quarter), 0)
    source = lax.broadcasted_iota(jnp.int32, (quarter, quarter), 1)
    wanted = (place % cols_each) * POINTS + place // cols_each
    pick_cols = jnp.where(source == wanted, 1.0, 0.0).astype(bf16)
    turned = lax.dot_general(
        pick_cols, ordered, (((1,), (1,)), ((), ())), preferred_element_type=f32
    ).astype(bf16)
    for j in range(n_half):
        for c in range(POINTS):
            y_ref[j, c] = turned[c * cols_each:(c + 1) * cols_each, j * share:(j + 1) * share]


def rows_kernel(n_rows, n_half, y_ref, hi_ref, lo_ref, tc_ref, ts_ref, z_ref, re_ref, im_ref):
    share = y_ref.shape[3]
    kept = z_ref.shape[1]
    span = z_ref.shape[3]

    def first(c, carry):
        block = jnp.concatenate([y_ref[j, c] for j in range(n_half)], axis=0).T
        both = dot(block, hi_ref[...]) + dot(block, lo_ref[...])
        re, im = both[:, :BOX], both[:, BOX:]
        tc, ts = tc_ref[c], ts_ref[c]
        re_ref[c] = re * tc + im * ts
        im_ref[c] = im * tc - re * ts
        return carry

    lax.fori_loop(0, POINTS, first, 0)
    tiles = span // 16

    def second(t, carry):
        m = t // tiles
        at = pl.multiple_of((t % tiles) * 16, 16)
        row = pl.multiple_of(t * 16, 16)
        for h in range(BOX // LANES):
            lanes = pl.ds(h * LANES, LANES)
            re = [re_ref[c, pl.ds(row, 16), lanes] for c in range(POINTS)]
            im = [im_ref[c, pl.ds(row, 16), lanes] for c in range(POINTS)]
            re, im = dft16(re, im)
            for v in range(POINTS):
                slab = v * (BOX // LANES) + h
                to = (slab % n_rows) * n_half + slab // n_rows
                z_ref[to, m, 0, pl.ds(at, 16), :] = re[v].astype(bf16)
                z_ref[to, m, 1, pl.ds(at, 16), :] = im[v].astype(bf16)
        return carry

    lax.fori_loop(0, share // 16, second, 0)


def columns_kernel(n_rows, n_half, z_ref, ahi_ref, alo_ref, bhi_ref, blo_ref, tc_ref, ts_ref,
                   o_ref, re_ref, im_ref):
    kept = z_ref.shape[1]
    count = o_ref.shape[0]

    def first(r, carry):
        j = r // kept
        m = r % kept
        real = jnp.concatenate([z_ref[i * n_half + j, m, 0] for i in range(n_rows)], axis=0).T
        imag = jnp.concatenate([z_ref[i * n_half + j, m, 1] for i in range(n_rows)], axis=0).T
        both = (dot(real, ahi_ref[...]) + dot(imag, bhi_ref[...])
                + dot(real, alo_ref[...]) + dot(imag, blo_ref[...]))
        re, im = both[:, :BOX], both[:, BOX:]
        tc, ts = tc_ref[r], ts_ref[r]
        re_ref[r] = re * tc + im * ts
        im_ref[r] = im * tc - re * ts
        return carry

    lax.fori_loop(0, POINTS, first, 0)

    def second(t, carry):
        row = pl.multiple_of(t * 8, 8)
        for h in range(BOX // LANES):
            lanes = pl.ds(h * LANES, LANES)
            re = [re_ref[c, pl.ds(row, 8), lanes] for c in range(POINTS)]
            im = [im_ref[c, pl.ds(row, 8), lanes] for c in range(POINTS)]
            re, im = dft16(re, im)
            for u in range(POINTS):
                o_ref[pl.ds(row, 8), pl.ds(u * BOX + h * LANES, LANES)] = re[u] * re[u] + im[u] * im[u]
        return carry

    lax.fori_loop(0, count // 8, second, 0)


def pieces_kernel(at_ref, x_ref, low_ref, o_ref, ext_ref):
    height, quarter = x_ref.shape
    tall, wide = height // BOX, quarter // BOX
    ext_ref[pl.ds(0, height), :] = x_ref[...]
    ext_ref[pl.ds(height, BOX), :] = low_ref[...]
    chunk = 64

    def one(slot, carry):
        top, left = at_ref[2 * slot], at_ref[2 * slot + 1]
        tile_row = jnp.clip(top >> 8, 0, tall - 1)
        tile_col = left >> 8
        row_cut, col_cut = top & (BOX - 1), left & (BOX - 1)
        here = jnp.logical_and(tile_col >= 0, tile_col < wide).astype(f32)
        after = jnp.logical_and(tile_col >= -1, tile_col < wide - 1).astype(f32)
        col_a = pl.multiple_of(jnp.clip(tile_col, 0, wide - 1) * BOX, BOX)
        col_b = pl.multiple_of(jnp.clip(tile_col + 1, 0, wide - 1) * BOX, BOX)
        right = lax.broadcasted_iota(jnp.int32, (chunk, BOX), 1) >= col_cut
        rows = lax.broadcasted_iota(jnp.int32, (chunk, BOX), 0)
        for k in range(BOX // chunk):
            upper = pl.multiple_of(tile_row * BOX + k * chunk, chunk)
            lower = pl.multiple_of(tile_row * BOX + BOX + k * chunk, chunk)

            def across(first_row):
                a = ext_ref[pl.ds(first_row, chunk), pl.ds(col_a, BOX)].astype(f32) * here
                b = ext_ref[pl.ds(first_row, chunk), pl.ds(col_b, BOX)].astype(f32) * after
                return jnp.where(right, a, b)

            whole = jnp.where(rows + k * chunk >= row_cut, across(upper), across(lower))
            o_ref[slot, pl.ds(k * chunk, chunk), :] = whole.astype(bf16)
        return carry

    lax.fori_loop(0, o_ref.shape[0], one, 0)


def spectra_kernel(n_rows, n_half, roll_ref, p_ref, whi_ref, wlo_ref, chi_ref, clo_ref, o_ref):
    slots = p_ref.shape[1]
    wide = 2 * BOX
    tall = BOX // n_rows
    band = wide // n_half

    def one(s, carry):
        box = p_ref[0, s].astype(f32)
        for j in range(1, n_half):
            box = box + p_ref[j, s].astype(f32)
        box = pltpu.roll(box, roll_ref[2 * s], 0)
        box = pltpu.roll(box, roll_ref[2 * s + 1], 1).astype(bf16)
        inner = dot(box, whi_ref[...]) + dot(box, wlo_ref[...])
        high = inner.astype(bf16)
        low = (inner - high.astype(f32)).astype(bf16)
        high = jnp.concatenate([high[:, :wide], high[:, wide:]], axis=0)
        low = jnp.concatenate([low[:, :wide], low[:, wide:]], axis=0)
        outer = dot(chi_ref[...], high) + dot(chi_ref[...], low) + dot(clo_ref[...], high)
        outer = outer.astype(bf16)
        for i in range(n_rows):
            for j in range(n_half):
                o_ref[i * n_half + j, s] = outer[i * tall:(i + 1) * tall, j * band:(j + 1) * band]
        return carry

    lax.fori_loop(0, slots, one, 0)


def means_kernel(label_ref, live_ref, f_ref, o_ref, sum_ref, count_ref):
    slots = f_ref.shape[1]
    half = f_ref.shape[3] // 2
    sum_ref[...] = jnp.zeros_like(sum_ref)

    def clear(k, carry):
        count_ref[k] = 0
        return carry

    lax.fori_loop(0, CLASSES, clear, 0)

    def add(g, carry):
        for s in range(slots):
            k = label_ref[g * slots + s]
            live = live_ref[g * slots + s]
            count_ref[k] = count_ref[k] + live
            sum_ref[k] = sum_ref[k] + f_ref[g, s].astype(f32) * live.astype(f32)
        return carry

    lax.fori_loop(0, f_ref.shape[0], add, 0)

    def finish(k, carry):
        mean = sum_ref[k] / jnp.maximum(count_ref[k], 1).astype(f32)
        o_ref[k, 0] = mean[:, :half]
        o_ref[k, 1] = mean[:, half:]
        return carry

    lax.fori_loop(0, CLASSES, finish, 0)


def fast_device(micrograph, box_tops, box_live, box_class, box_shift):
    n_rows = lax.axis_size("rows")
    n_half = lax.axis_size("half")
    everyone = ("rows", "half")
    total = n_rows * n_half
    height, quarter = micrograph.shape
    width = quarter * n_half
    row_index = lax.axis_index("rows")
    half_index = lax.axis_index("half")
    kept = POINTS // n_half
    span = height // POINTS
    slab = quarter // n_rows
    slots = box_tops.shape[2]
    shape = jax.ShapeDtypeStruct

    below = passed_along(micrograph[:BOX], "rows", -1)

    points = np.arange(BOX)
    cos_box, sin_box = waves(points, points, BOX)
    first_hi, first_lo = halves(np.concatenate([cos_box, -sin_box], axis=1))
    turned_hi, turned_lo = halves(np.concatenate([sin_box, cos_box], axis=1))
    tc, ts = waves(np.arange(POINTS), points, width)
    tc = tc.astype(np.float32)[:, None, :]
    ts = ts.astype(np.float32)[:, None, :]

    ready = call(
        functools.partial(prepare_kernel, n_half),
        shape((n_half, POINTS, quarter // POINTS, height // n_half), bf16),
        [micrograph], [VMEM],
        flops=2 * height * quarter * (height + quarter),
    )
    ready = lax.all_to_all(ready, "half", 0, 0, tiled=True)
    mixed = call(
        functools.partial(rows_kernel, n_rows, n_half),
        shape((total, kept, 2, span, slab), bf16),
        [ready, first_hi, first_lo, tc, ts], [VMEM] * 5,
        scratch=[pltpu.VMEM((POINTS, height // n_half, BOX), f32)] * 2,
        flops=4 * height * quarter * 2 * BOX,
    )
    mixed = lax.all_to_all(mixed, everyone, 0, 0, tiled=True)

    corner = jnp.stack([row_index * height, half_index * quarter])
    at = (box_tops[row_index] - corner).reshape(-1)
    pieces = call(
        pieces_kernel,
        shape((n_half * slots, BOX, BOX), bf16),
        [at, micrograph, below], [SMEM, VMEM, VMEM],
        scratch=[pltpu.VMEM((height + BOX, quarter), bf16)],
        flops=10 * n_half * slots * BOX * BOX,
    )
    pieces = lax.all_to_all(pieces, "half", 0, 0, tiled=True).reshape(n_half, slots, BOX, BOX)
    part = BOX // n_half

    def by_part(a, b):
        a = a.reshape(-1, n_half, 1, part)
        b = b.reshape(-1, n_half, 1, part)
        return np.concatenate([a, b], axis=2).reshape(-1, 2 * BOX)

    plain = by_part(cos_box, -sin_box)
    swapped = by_part(-sin_box, -cos_box)
    inner_hi, inner_lo = halves(np.concatenate([plain, swapped], axis=1) / BOX)
    outer_hi, outer_lo = halves(np.concatenate([cos_box, sin_box], axis=1))
    my_tops = box_tops[row_index, half_index]
    rolls = jnp.mod(box_shift.reshape(slots, 2) - my_tops, BOX).reshape(-1)
    spectra = call(
        functools.partial(spectra_kernel, n_rows, n_half),
        shape((total, slots, BOX // n_rows, 2 * part), bf16),
        [rolls, pieces, inner_hi, inner_lo, outer_hi, outer_lo], [SMEM] + [VMEM] * 5,
        flops=slots * BOX * BOX * 4 * BOX * 10,
    )
    spectra = lax.all_to_all(spectra, everyone, 0, 0, tiled=True)

    power = call(
        functools.partial(columns_kernel, n_rows, n_half),
        shape((slab, width), f32),
        [mixed, first_hi, first_lo, turned_hi, turned_lo, tc / width, ts / width], [VMEM] * 7,
        scratch=[pltpu.VMEM((POINTS, slab, BOX), f32)] * 2,
        flops=8 * slab * width * 2 * BOX,
    )[None]
    class_means = call(
        means_kernel,
        shape((CLASSES, 2, BOX // n_rows, part), f32),
        [box_class.reshape(-1), box_live.reshape(-1), spectra], [SMEM, SMEM, VMEM],
        scratch=[pltpu.VMEM((CLASSES, BOX // n_rows, 2 * part), f32), pltpu.SMEM((CLASSES,), jnp.int32)],
        flops=4 * total * slots * BOX * BOX,
    )
    return (power, class_means)


def fits(mesh, micrograph):
    height, quarter = micrograph.shape
    n_rows, n_half = mesh.shape["rows"], mesh.shape["half"]
    return (
        height * n_rows == POINTS * BOX
        and quarter * n_half == POINTS * BOX
        and POINTS % n_half == 0
        and height % BOX == 0
        and quarter % BOX == 0
        and height // n_half == LANES
        and quarter // n_rows == LANES
        and BOX // n_rows % 16 == 0
        and 2 * BOX // n_half == LANES
    )


def solution(mesh):
    in_specs = (P("rows", "half"), P(), P(), P(), P("rows", "half", None, None))
    out_specs = (P("half", "rows", None), P(None, None, "rows", "half"))

    def per_device(micrograph, *boxes):
        device = fast_device if fits(mesh, micrograph) else general_device
        return device(micrograph, *boxes)

    return jax.shard_map(
        per_device, mesh=mesh, in_specs=in_specs, out_specs=out_specs, check_vma=False
    )
```

```python
import functools

import numpy as np

import jax
import jax.numpy as jnp
from jax import lax
from jax.experimental import pallas as pl
from jax.experimental.pallas import tpu as pltpu
from jax.sharding import PartitionSpec as P

BOX = 256
CLASSES = 50
RADIX = 64
LANES = 128
POINTS = 16

highest = lax.Precision.HIGHEST


def passed_along(block, axis, distance):
    devices = range(lax.axis_size(axis))
    route = [(i - distance, i) for i in devices if i - distance in devices]
    return lax.ppermute(block, axis, route)


def phases(left_index, right_index, length):
    rotations = jnp.mod(left_index[:, None] * right_index[None, :], length)
    angles = 2.0 * jnp.pi / length * rotations.astype(jnp.float32)
    return (jnp.cos(angles), jnp.sin(angles))


def product(pattern, left_side, matrix):
    return jnp.einsum(pattern, left_side, matrix, precision=highest)


def four_step(real_part, imag_part, first_index, how_many, rows_last):
    height = real_part.shape[0]
    length = real_part.shape[1]
    outer_size = RADIX
    inner_size = length // outer_size
    real_part = real_part.reshape(height, outer_size, inner_size)
    spread = jnp.arange(outer_size, dtype=jnp.int32)
    across = jnp.arange(inner_size, dtype=jnp.int32)
    cos_one, sin_one = phases(spread, spread, outer_size)
    section_real = product("mab,ka->mkb", real_part, cos_one)
    section_imag = -product("mab,ka->mkb", real_part, sin_one)
    if imag_part is not None:
        imag_part = imag_part.reshape(height, outer_size, inner_size)
        section_real = section_real + product("mab,ka->mkb", imag_part, sin_one)
        section_imag = section_imag + product("mab,ka->mkb", imag_part, cos_one)
    twist_cos, twist_sin = phases(spread, across, length)
    turned_real = section_real * twist_cos + section_imag * twist_sin
    turned_imag = section_imag * twist_cos - section_real * twist_sin
    wanted = first_index + jnp.arange(how_many, dtype=jnp.int32)
    cos_two, sin_two = phases(wanted, across, inner_size)
    pattern = "mkb,tb->tkm" if rows_last else "mkb,tb->mtk"
    out_real = product(pattern, turned_real, cos_two) + product(pattern, turned_imag, sin_two)
    out_imag = product(pattern, turned_imag, cos_two) - product(pattern, turned_real, sin_two)
    return (out_real, out_imag)


def general_device(micrograph, box_tops, box_live, box_class, box_shift):
    row_index = lax.axis_index("rows")
    half_index = lax.axis_index("half")
    band_rows = lax.all_gather(micrograph, "half", axis=1, tiled=True)
    height = band_rows.shape[0]
    full_width = band_rows.shape[1]
    quarter = full_width // lax.axis_size("half")
    per_block = quarter // RADIX
    image_rows = band_rows.astype(jnp.float32)
    part_real, part_imag = four_step(image_rows, None, half_index * per_block, per_block, True)
    partial_value = jnp.stack(
        [part_real.reshape(quarter, height), part_imag.reshape(quarter, height)]
    )
    columns = lax.all_to_all(partial_value, "rows", split_axis=1, concat_axis=2, tiled=True)
    column_count = columns.shape[1]
    freq_real, freq_imag = four_step(columns[0], columns[1], 0, full_width // RADIX, False)
    power_out = (freq_real * freq_real + freq_imag * freq_imag).reshape(1, column_count, full_width)
    power_out = power_out / (full_width * full_width)
    local_tops = box_tops[row_index, half_index]
    start_rows = local_tops[:, 0] - row_index * height
    start_cols = local_tops[:, 1]
    reach_bands = (BOX + height - 2) // height

    def cut_columns(source, corner):
        return lax.dynamic_slice_in_dim(source, corner, BOX, 1)

    pieces = [jax.vmap(cut_columns, (None, 0))(band_rows, start_cols)]
    for offset in range(1, reach_bands + 1):
        target = jnp.maximum(row_index - offset, 0)
        their_cols = box_tops[target, half_index][:, 1]
        outgoing = jax.vmap(cut_columns, (None, 0))(band_rows, their_cols)
        pieces.append(passed_along(outgoing, "rows", -offset))
    windows = jnp.concatenate(pieces, axis=1)
    particle_boxes = jax.vmap(
        lambda window, corner: lax.dynamic_slice_in_dim(window, corner, BOX, 0)
    )(windows, start_rows)
    frequency = jnp.arange(BOX, dtype=jnp.int32)
    cos_box, sin_box = phases(frequency, frequency, BOX)
    local_offsets = box_shift.reshape(-1, 2)

    def spectrum(member):
        particle, offsets_pair = member
        values = particle.astype(jnp.float32)
        inner_real = jnp.dot(values, cos_box, precision=highest)
        inner_imag = -jnp.dot(values, sin_box, precision=highest)
        outer_real = (
            jnp.dot(cos_box, inner_real, precision=highest)
            + jnp.dot(sin_box, inner_imag, precision=highest)
        ) / BOX
        outer_imag = (
            jnp.dot(cos_box, inner_imag, precision=highest)
            - jnp.dot(sin_box, inner_real, precision=highest)
        ) / BOX
        rotations = jnp.mod(
            frequency[:, None] * offsets_pair[0] + frequency[None, :] * offsets_pair[1], BOX
        )
        angles = 2.0 * jnp.pi / BOX * rotations.astype(jnp.float32)
        ramp_cos = jnp.cos(angles)
        ramp_sin = jnp.sin(angles)
        shifted_real = outer_real * ramp_cos + outer_imag * ramp_sin
        shifted_imag = outer_imag * ramp_cos - outer_real * ramp_sin
        return jnp.stack([shifted_real, shifted_imag]).astype(jnp.bfloat16)

    spectra = lax.map(spectrum, (particle_boxes, local_offsets))
    classes_all = jnp.arange(CLASSES, dtype=jnp.int32)
    all_labels = box_class.reshape(-1)
    all_live = box_live.reshape(-1)
    counts = jnp.sum(
        (all_labels[None, :] == classes_all[:, None]).astype(jnp.int32) * all_live[None, :], axis=1
    )
    arrived = lax.all_to_all(spectra, "rows", split_axis=2, concat_axis=0, tiled=True)
    chosen_labels = box_class[:, half_index].reshape(-1)
    chosen_live = box_live[:, half_index].reshape(-1)
    weights = (
        (chosen_labels[None, :] == classes_all[:, None]).astype(jnp.int32) * chosen_live[None, :]
    ).astype(jnp.bfloat16)
    flat_spectra = arrived.reshape(arrived.shape[0], -1)
    partial_sums = jnp.dot(weights, flat_spectra, preferred_element_type=jnp.float32)
    partial_sums = partial_sums.reshape((CLASSES,) + arrived.shape[1:])
    class_sums = lax.psum_scatter(partial_sums, "half", scatter_dimension=3, tiled=True)
    divisor = jnp.maximum(counts, 1).astype(jnp.float32)
    class_means = class_sums / divisor[:, None, None, None]
    return (power_out, class_means)


f32 = jnp.float32
bf16 = jnp.bfloat16
VMEM = pl.BlockSpec(memory_space=pltpu.VMEM)
SMEM = pl.BlockSpec(memory_space=pltpu.SMEM)


def call(kernel, out, operands, specs, scratch=(), flops=0):
    moved = sum(a.size * a.dtype.itemsize for a in operands) + out.size * out.dtype.itemsize
    return pl.pallas_call(
        kernel,
        out_shape=out,
        in_specs=specs,
        out_specs=VMEM,
        scratch_shapes=list(scratch),
        compiler_params=pltpu.CompilerParams(vmem_limit_bytes=48 * 1024 * 1024),
        cost_estimate=pl.CostEstimate(flops=flops, bytes_accessed=moved, transcendentals=0),
    )(*operands)


def halves(table):
    high = table.astype(bf16)
    low = (table - high.astype(np.float64)).astype(bf16)
    return high, low


def waves(left, right, length):
    angles = 2.0 * np.pi / length * np.mod(np.outer(left, right), length)
    return np.cos(angles), np.sin(angles)


def dft4(re, im):
    sr, si = re[0] + re[2], im[0] + im[2]
    dr, di = re[0] - re[2], im[0] - im[2]
    tr, ti = re[1] + re[3], im[1] + im[3]
    er, ei = re[1] - re[3], im[1] - im[3]
    return [sr + tr, dr + ei, sr - tr, dr - ei], [si + ti, di - er, si - ti, di + er]


def turn(re, im, step):
    step = step % POINTS
    if step == 0:
        return re, im
    if step == POINTS // 4:
        return im, -re
    c = float(np.cos(2.0 * np.pi * step / POINTS))
    s = float(np.sin(2.0 * np.pi * step / POINTS))
    if step == POINTS // 8:
        return (re + im) * c, (im - re) * c
    if step == 3 * POINTS // 8:
        return (im - re) * s, (re + im) * -s
    return re * c + im * s, im * c - re * s


def dft16(re, im):
    mid_re = [[None] * 4 for _ in range(4)]
    mid_im = [[None] * 4 for _ in range(4)]
    for n in range(4):
        yr, yi = dft4([re[4 * p + n] for p in range(4)], [im[4 * p + n] for p in range(4)])
        for k in range(4):
            mid_re[k][n], mid_im[k][n] = turn(yr[k], yi[k], n * k)
    out_re, out_im = [None] * POINTS, [None] * POINTS
    for k in range(4):
        yr, yi = dft4(mid_re[k], mid_im[k])
        for m in range(4):
            out_re[k + 4 * m], out_im[k + 4 * m] = yr[m], yi[m]
    return out_re, out_im


def dot(a, b):
    return jnp.dot(a, b, preferred_element_type=f32)


def prepare_kernel(n_half, x_ref, y_ref):
    height, quarter = x_ref.shape
    rows_each = height // POINTS
    kept = POINTS // n_half
    cols_each = quarter // POINTS
    share = height // n_half
    place = lax.broadcasted_iota(jnp.int32, (height, height), 0)
    source = lax.broadcasted_iota(jnp.int32, (height, height), 1)
    wanted = (place % rows_each) * POINTS + place // rows_each
    pick_rows = jnp.where(source == wanted, 1.0, 0.0).astype(bf16)
    ordered = dot(pick_rows, x_ref[...]).astype(bf16)
    place = lax.broadcasted_iota(jnp.int32, (quarter, quarter), 0)
    source = lax.broadcasted_iota(jnp.int32, (quarter, quarter), 1)
    wanted = (place % cols_each) * POINTS + place // cols_each
    pick_cols = jnp.where(source == wanted, 1.0, 0.0).astype(bf16)
    turned = lax.dot_general(
        pick_cols, ordered, (((1,), (1,)), ((), ())), preferred_element_type=f32
    ).astype(bf16)
    for j in range(n_half):
        for c in range(POINTS):
            y_ref[j, c] = turned[c * cols_each:(c + 1) * cols_each, j * share:(j + 1) * share]


def rows_kernel(n_rows, n_half, y_ref, hi_ref, lo_ref, tc_ref, ts_ref, z_ref, re_ref, im_ref):
    share = y_ref.shape[3]
    kept = z_ref.shape[1]
    span = z_ref.shape[3]

    def first(c, carry):
        block = jnp.concatenate([y_ref[j, c] for j in range(n_half)], axis=0).T
        both = dot(block, hi_ref[...]) + dot(block, lo_ref[...])
        re, im = both[:, :BOX], both[:, BOX:]
        tc, ts = tc_ref[c], ts_ref[c]
        re_ref[c] = re * tc + im * ts
        im_ref[c] = im * tc - re * ts
        return carry

    lax.fori_loop(0, POINTS, first, 0)
    tiles = span // 16

    def second(t, carry):
        m = t // tiles
        at = pl.multiple_of((t % tiles) * 16, 16)
        row = pl.multiple_of(t * 16, 16)
        for h in range(BOX // LANES):
            lanes = pl.ds(h * LANES, LANES)
            re = [re_ref[c, pl.ds(row, 16), lanes] for c in range(POINTS)]
            im = [im_ref[c, pl.ds(row, 16), lanes] for c in range(POINTS)]
            re, im = dft16(re, im)
            for v in range(POINTS):
                slab = v * (BOX // LANES) + h
                to = (slab % n_rows) * n_half + slab // n_rows
                z_ref[to, m, 0, pl.ds(at, 16), :] = re[v].astype(bf16)
                z_ref[to, m, 1, pl.ds(at, 16), :] = im[v].astype(bf16)
        return carry

    lax.fori_loop(0, share // 16, second, 0)


def columns_kernel(n_rows, n_half, z_ref, ahi_ref, alo_ref, bhi_ref, blo_ref, tc_ref, ts_ref,
                   o_ref, re_ref, im_ref):
    kept = z_ref.shape[1]
    count = o_ref.shape[0]

    def first(r, carry):
        j = r // kept
        m = r % kept
        real = jnp.concatenate([z_ref[i * n_half + j, m, 0] for i in range(n_rows)], axis=0).T
        imag = jnp.concatenate([z_ref[i * n_half + j, m, 1] for i in range(n_rows)], axis=0).T
        both = (dot(real, ahi_ref[...]) + dot(imag, bhi_ref[...])
                + dot(real, alo_ref[...]) + dot(imag, blo_ref[...]))
        re, im = both[:, :BOX], both[:, BOX:]
        tc, ts = tc_ref[r], ts_ref[r]
        re_ref[r] = re * tc + im * ts
        im_ref[r] = im * tc - re * ts
        return carry

    lax.fori_loop(0, POINTS, first, 0)

    def second(t, carry):
        row = pl.multiple_of(t * 8, 8)
        for h in range(BOX // LANES):
            lanes = pl.ds(h * LANES, LANES)
            re = [re_ref[c, pl.ds(row, 8), lanes] for c in range(POINTS)]
            im = [im_ref[c, pl.ds(row, 8), lanes] for c in range(POINTS)]
            re, im = dft16(re, im)
            for u in range(POINTS):
                o_ref[pl.ds(row, 8), pl.ds(u * BOX + h * LANES, LANES)] = re[u] * re[u] + im[u] * im[u]
        return carry

    lax.fori_loop(0, count // 8, second, 0)


def pieces_kernel(at_ref, x_ref, low_ref, o_ref, ext_ref):
    height, quarter = x_ref.shape
    tall, wide = height // BOX, quarter // BOX
    ext_ref[pl.ds(0, height), :] = x_ref[...]
    ext_ref[pl.ds(height, BOX), :] = low_ref[...]
    chunk = 64
    slots = o_ref.shape[1]

    def one(slot, carry):
        top, left = at_ref[2 * slot], at_ref[2 * slot + 1]
        tile_row = jnp.clip(top >> 8, 0, tall - 1)
        tile_col = left >> 8
        row_cut, col_cut = top & (BOX - 1), left & (BOX - 1)
        here = jnp.logical_and(tile_col >= 0, tile_col < wide).astype(f32)
        after = jnp.logical_and(tile_col >= -1, tile_col < wide - 1).astype(f32)
        col_a = pl.multiple_of(jnp.clip(tile_col, 0, wide - 1) * BOX, BOX)
        col_b = pl.multiple_of(jnp.clip(tile_col + 1, 0, wide - 1) * BOX, BOX)
        right = lax.broadcasted_iota(jnp.int32, (chunk, BOX), 1) >= col_cut
        rows = lax.broadcasted_iota(jnp.int32, (chunk, BOX), 0)
        for k in range(BOX // chunk):
            upper = pl.multiple_of(tile_row * BOX + k * chunk, chunk)
            lower = pl.multiple_of(tile_row * BOX + BOX + k * chunk, chunk)

            def across(first_row):
                a = ext_ref[pl.ds(first_row, chunk), pl.ds(col_a, BOX)].astype(f32) * here
                b = ext_ref[pl.ds(first_row, chunk), pl.ds(col_b, BOX)].astype(f32) * after
                return jnp.where(right, a, b)

            whole = jnp.where(rows + k * chunk >= row_cut, across(upper), across(lower))
            o_ref[slot // slots, slot % slots, pl.ds(k * chunk, chunk), :] = whole.astype(bf16)
        return carry

    lax.fori_loop(0, o_ref.shape[0] * slots, one, 0)


def spectra_kernel(n_rows, n_half, roll_ref, p_ref, q_ref, r_ref, whi_ref, wlo_ref, chi_ref, clo_ref, o_ref):
    slots = q_ref.shape[0]
    wide = 2 * BOX
    tall = BOX // n_rows
    band = wide // n_half

    def one(s, carry):
        box = p_ref[s].astype(f32) + q_ref[s].astype(f32) + r_ref[s].astype(f32)
        box = pltpu.roll(box, roll_ref[2 * s], 0)
        box = pltpu.roll(box, roll_ref[2 * s + 1], 1).astype(bf16)
        inner = dot(box, whi_ref[...]) + dot(box, wlo_ref[...])
        high = inner.astype(bf16)
        low = (inner - high.astype(f32)).astype(bf16)
        high = jnp.concatenate([high[:, :wide], high[:, wide:]], axis=0)
        low = jnp.concatenate([low[:, :wide], low[:, wide:]], axis=0)
        outer = dot(chi_ref[...], high) + dot(chi_ref[...], low) + dot(clo_ref[...], high)
        outer = outer.astype(bf16)
        for i in range(n_rows):
            for j in range(n_half):
                o_ref[i * n_half + j, s] = outer[i * tall:(i + 1) * tall, j * band:(j + 1) * band]
        return carry

    lax.fori_loop(0, slots, one, 0)


def means_kernel(label_ref, live_ref, divisor_ref, f_ref, o_ref, *sum_refs):
    slots = f_ref.shape[1]
    half = f_ref.shape[3] // 2
    for sum_ref in sum_refs:
        sum_ref[...] = jnp.zeros_like(sum_ref)

    def add(g, carry):
        for s, sum_ref in enumerate(sum_refs):
            k = label_ref[g * slots + s]
            live = live_ref[g * slots + s].astype(f32)
            sum_ref[k] = sum_ref[k] + f_ref[g, s].astype(f32) * live
        return carry

    lax.fori_loop(0, f_ref.shape[0], add, 0)

    def finish(k, carry):
        mean = sum_refs[0][k]
        for sum_ref in sum_refs[1:]:
            mean = mean + sum_ref[k]
        mean = mean / divisor_ref[k]
        o_ref[k, 0] = mean[:, :half]
        o_ref[k, 1] = mean[:, half:]
        return carry

    lax.fori_loop(0, o_ref.shape[0], finish, 0)


def swapped(block, axis, bit):
    route = [(i, i ^ bit) for i in range(lax.axis_size(axis))]
    return lax.ppermute(block, axis, route)


def fast_device(micrograph, box_tops, box_live, box_class, box_shift):
    n_rows = lax.axis_size("rows")
    n_half = lax.axis_size("half")
    everyone = ("rows", "half")
    total = n_rows * n_half
    height, quarter = micrograph.shape
    width = quarter * n_half
    row_index = lax.axis_index("rows")
    half_index = lax.axis_index("half")
    kept = POINTS // n_half
    span = height // POINTS
    slab = quarter // n_rows
    slots = box_tops.shape[2]
    shape = jax.ShapeDtypeStruct

    below = passed_along(micrograph[:BOX], "rows", -1)

    points = np.arange(BOX)
    cos_box, sin_box = waves(points, points, BOX)
    first_hi, first_lo = halves(np.concatenate([cos_box, -sin_box], axis=1))
    turned_hi, turned_lo = halves(np.concatenate([sin_box, cos_box], axis=1))
    tc, ts = waves(np.arange(POINTS), points, width)
    tc = tc.astype(np.float32)[:, None, :]
    ts = ts.astype(np.float32)[:, None, :]

    ready = call(
        functools.partial(prepare_kernel, n_half),
        shape((n_half, POINTS, quarter // POINTS, height // n_half), bf16),
        [micrograph], [VMEM],
        flops=2 * height * quarter * (height + quarter),
    )
    ready = lax.all_to_all(ready, "half", 0, 0, tiled=True)
    mixed = call(
        functools.partial(rows_kernel, n_rows, n_half),
        shape((total, kept, 2, span, slab), bf16),
        [ready, first_hi, first_lo, tc, ts], [VMEM] * 5,
        scratch=[pltpu.VMEM((POINTS, height // n_half, BOX), f32)] * 2,
        flops=4 * height * quarter * 2 * BOX,
    )
    mixed = lax.all_to_all(mixed, everyone, 0, 0, tiled=True)

    corner = jnp.stack([row_index * height, half_index * quarter])
    owners = jnp.bitwise_xor(half_index, jnp.asarray(np.array([0, 2, 1, 3], np.int32)))
    at = (box_tops[row_index][owners] - corner).reshape(-1)
    pieces = call(
        pieces_kernel,
        shape((n_half, slots, BOX, BOX), bf16),
        [at, micrograph, below], [SMEM, VMEM, VMEM],
        scratch=[pltpu.VMEM((height + BOX, quarter), bf16)],
        flops=10 * n_half * slots * BOX * BOX,
    )
    beside = swapped(pieces[2:], "half", 1)
    across = swapped(pieces[1] + beside[1], "half", 2)
    part = BOX // n_half

    def by_part(a, b):
        a = a.reshape(-1, n_half, 1, part)
        b = b.reshape(-1, n_half, 1, part)
        return np.concatenate([a, b], axis=2).reshape(-1, 2 * BOX)

    plain = by_part(cos_box, -sin_box)
    crossed = by_part(-sin_box, -cos_box)
    inner_hi, inner_lo = halves(np.concatenate([plain, crossed], axis=1) / BOX)
    outer_hi, outer_lo = halves(np.concatenate([cos_box, sin_box], axis=1))
    my_tops = box_tops[row_index, half_index]
    rolls = jnp.mod(box_shift.reshape(slots, 2) - my_tops, BOX).reshape(-1)
    spectra = call(
        functools.partial(spectra_kernel, n_rows, n_half),
        shape((total, slots, BOX // n_rows, 2 * part), bf16),
        [rolls, pieces[0], beside[0], across, inner_hi, inner_lo, outer_hi, outer_lo], [SMEM] + [VMEM] * 7,
        flops=slots * BOX * BOX * 4 * BOX * 10,
    )
    spectra, mixed = lax.optimization_barrier((spectra, mixed))
    spectra = lax.all_to_all(spectra, everyone, 0, 0, tiled=True)

    power = call(
        functools.partial(columns_kernel, n_rows, n_half),
        shape((slab, width), f32),
        [mixed, first_hi, first_lo, turned_hi, turned_lo, tc / width, ts / width], [VMEM] * 7,
        scratch=[pltpu.VMEM((POINTS, slab, BOX), f32)] * 2,
        flops=8 * slab * width * 2 * BOX,
    )[None]
    labels, lives = box_class.reshape(-1), box_live.reshape(-1)
    matches = labels[None, :] == jnp.arange(CLASSES, dtype=jnp.int32)[:, None]
    counts = jnp.sum(jnp.where(matches, lives[None, :], 0), axis=1)
    divisor = jnp.maximum(counts, 1).astype(f32)
    class_means = call(
        means_kernel,
        shape((CLASSES, 2, BOX // n_rows, part), f32),
        [labels, lives, divisor, spectra], [SMEM, SMEM, SMEM, VMEM],
        scratch=[pltpu.VMEM((CLASSES, BOX // n_rows, 2 * part), f32)] * slots,
        flops=4 * total * slots * BOX * BOX,
    )
    return (power, class_means)


def fits(mesh, micrograph):
    height, quarter = micrograph.shape
    n_rows, n_half = mesh.shape["rows"], mesh.shape["half"]
    return (
        height * n_rows == POINTS * BOX
        and quarter * n_half == POINTS * BOX
        and n_half == 4
        and height % BOX == 0
        and quarter % BOX == 0
        and height // n_half == LANES
        and quarter // n_rows == LANES
        and BOX // n_rows % 16 == 0
        and 2 * BOX // n_half == LANES
    )


def solution(mesh):
    in_specs = (P("rows", "half"), P(), P(), P(), P("rows", "half", None, None))
    out_specs = (P("half", "rows", None), P(None, None, "rows", "half"))

    def per_device(micrograph, *boxes):
        device = fast_device if fits(mesh, micrograph) else general_device
        return device(micrograph, *boxes)

    return jax.shard_map(
        per_device, mesh=mesh, in_specs=in_specs, out_specs=out_specs, check_vma=False
    )
```

```python
import functools

import numpy as np

import jax
import jax.numpy as jnp
from jax import lax
from jax.experimental import pallas as pl
from jax.experimental.pallas import tpu as pltpu
from jax.sharding import PartitionSpec as P


BOX = 256
CLASSES = 50
RADIX = 64
LANES = 128
POINTS = 16

highest = lax.Precision.HIGHEST


def passed_along(block, axis, distance):
    devices = range(lax.axis_size(axis))
    route = [(i - distance, i) for i in devices if i - distance in devices]
    return lax.ppermute(block, axis, route)


def phases(left_index, right_index, length):
    rotations = jnp.mod(left_index[:, None] * right_index[None, :], length)
    angles = 2.0 * jnp.pi / length * rotations.astype(jnp.float32)
    return (jnp.cos(angles), jnp.sin(angles))


def product(pattern, left_side, matrix):
    return jnp.einsum(pattern, left_side, matrix, precision=highest)


def four_step(real_part, imag_part, first_index, how_many, rows_last):
    height = real_part.shape[0]
    length = real_part.shape[1]
    outer_size = RADIX
    inner_size = length // outer_size
    real_part = real_part.reshape(height, outer_size, inner_size)
    spread = jnp.arange(outer_size, dtype=jnp.int32)
    across = jnp.arange(inner_size, dtype=jnp.int32)
    cos_one, sin_one = phases(spread, spread, outer_size)
    section_real = product("mab,ka->mkb", real_part, cos_one)
    section_imag = -product("mab,ka->mkb", real_part, sin_one)
    if imag_part is not None:
        imag_part = imag_part.reshape(height, outer_size, inner_size)
        section_real = section_real + product("mab,ka->mkb", imag_part, sin_one)
        section_imag = section_imag + product("mab,ka->mkb", imag_part, cos_one)
    twist_cos, twist_sin = phases(spread, across, length)
    turned_real = section_real * twist_cos + section_imag * twist_sin
    turned_imag = section_imag * twist_cos - section_real * twist_sin
    wanted = first_index + jnp.arange(how_many, dtype=jnp.int32)
    cos_two, sin_two = phases(wanted, across, inner_size)
    pattern = "mkb,tb->tkm" if rows_last else "mkb,tb->mtk"
    out_real = product(pattern, turned_real, cos_two) + product(pattern, turned_imag, sin_two)
    out_imag = product(pattern, turned_imag, cos_two) - product(pattern, turned_real, sin_two)
    return (out_real, out_imag)


def general_device(micrograph, box_tops, box_live, box_class, box_shift):
    row_index = lax.axis_index("rows")
    half_index = lax.axis_index("half")
    band_rows = lax.all_gather(micrograph, "half", axis=1, tiled=True)
    height = band_rows.shape[0]
    full_width = band_rows.shape[1]
    quarter = full_width // lax.axis_size("half")
    per_block = quarter // RADIX
    image_rows = band_rows.astype(jnp.float32)
    part_real, part_imag = four_step(image_rows, None, half_index * per_block, per_block, True)
    partial_value = jnp.stack(
        [part_real.reshape(quarter, height), part_imag.reshape(quarter, height)]
    )
    columns = lax.all_to_all(partial_value, "rows", split_axis=1, concat_axis=2, tiled=True)
    column_count = columns.shape[1]
    freq_real, freq_imag = four_step(columns[0], columns[1], 0, full_width // RADIX, False)
    power_out = (freq_real * freq_real + freq_imag * freq_imag).reshape(1, column_count, full_width)
    power_out = power_out / (full_width * full_width)
    local_tops = box_tops[row_index, half_index]
    start_rows = local_tops[:, 0] - row_index * height
    start_cols = local_tops[:, 1]
    reach_bands = (BOX + height - 2) // height

    def cut_columns(source, corner):
        return lax.dynamic_slice_in_dim(source, corner, BOX, 1)

    pieces = [jax.vmap(cut_columns, (None, 0))(band_rows, start_cols)]
    for offset in range(1, reach_bands + 1):
        target = jnp.maximum(row_index - offset, 0)
        their_cols = box_tops[target, half_index][:, 1]
        outgoing = jax.vmap(cut_columns, (None, 0))(band_rows, their_cols)
        pieces.append(passed_along(outgoing, "rows", -offset))
    windows = jnp.concatenate(pieces, axis=1)
    particle_boxes = jax.vmap(
        lambda window, corner: lax.dynamic_slice_in_dim(window, corner, BOX, 0)
    )(windows, start_rows)
    frequency = jnp.arange(BOX, dtype=jnp.int32)
    cos_box, sin_box = phases(frequency, frequency, BOX)
    local_offsets = box_shift.reshape(-1, 2)

    def spectrum(member):
        particle, offsets_pair = member
        values = particle.astype(jnp.float32)
        inner_real = jnp.dot(values, cos_box, precision=highest)
        inner_imag = -jnp.dot(values, sin_box, precision=highest)
        outer_real = (
            jnp.dot(cos_box, inner_real, precision=highest)
            + jnp.dot(sin_box, inner_imag, precision=highest)
        ) / BOX
        outer_imag = (
            jnp.dot(cos_box, inner_imag, precision=highest)
            - jnp.dot(sin_box, inner_real, precision=highest)
        ) / BOX
        rotations = jnp.mod(
            frequency[:, None] * offsets_pair[0] + frequency[None, :] * offsets_pair[1], BOX
        )
        angles = 2.0 * jnp.pi / BOX * rotations.astype(jnp.float32)
        ramp_cos = jnp.cos(angles)
        ramp_sin = jnp.sin(angles)
        shifted_real = outer_real * ramp_cos + outer_imag * ramp_sin
        shifted_imag = outer_imag * ramp_cos - outer_real * ramp_sin
        return jnp.stack([shifted_real, shifted_imag]).astype(jnp.bfloat16)

    spectra = lax.map(spectrum, (particle_boxes, local_offsets))
    classes_all = jnp.arange(CLASSES, dtype=jnp.int32)
    all_labels = box_class.reshape(-1)
    all_live = box_live.reshape(-1)
    counts = jnp.sum(
        (all_labels[None, :] == classes_all[:, None]).astype(jnp.int32) * all_live[None, :], axis=1
    )
    arrived = lax.all_to_all(spectra, "rows", split_axis=2, concat_axis=0, tiled=True)
    chosen_labels = box_class[:, half_index].reshape(-1)
    chosen_live = box_live[:, half_index].reshape(-1)
    weights = (
        (chosen_labels[None, :] == classes_all[:, None]).astype(jnp.int32) * chosen_live[None, :]
    ).astype(jnp.bfloat16)
    flat_spectra = arrived.reshape(arrived.shape[0], -1)
    partial_sums = jnp.dot(weights, flat_spectra, preferred_element_type=jnp.float32)
    partial_sums = partial_sums.reshape((CLASSES,) + arrived.shape[1:])
    class_sums = lax.psum_scatter(partial_sums, "half", scatter_dimension=3, tiled=True)
    divisor = jnp.maximum(counts, 1).astype(jnp.float32)
    class_means = class_sums / divisor[:, None, None, None]
    return (power_out, class_means)


GROUP = 4
f32 = jnp.float32
bf16 = jnp.bfloat16
VMEM = pl.BlockSpec(memory_space=pltpu.VMEM)
SMEM = pl.BlockSpec(memory_space=pltpu.SMEM)
HBM = pl.BlockSpec(memory_space=pltpu.HBM)


def call(kernel, out, operands, specs, scratch=(), flops=0):
    made = out if isinstance(out, tuple) else (out,)
    moved = sum(a.size * a.dtype.itemsize for a in (*operands, *made))
    return pl.pallas_call(
        kernel,
        out_shape=out,
        in_specs=specs,
        out_specs=(VMEM,) * len(out) if isinstance(out, tuple) else VMEM,
        scratch_shapes=list(scratch),
        compiler_params=pltpu.CompilerParams(vmem_limit_bytes=48 * 1024 * 1024),
        cost_estimate=pl.CostEstimate(flops=flops, bytes_accessed=moved, transcendentals=0),
    )(*operands)


def halves(table):
    high = table.astype(bf16)
    low = (table - high.astype(np.float64)).astype(bf16)
    return high, low


def waves(left, right, length):
    angles = 2.0 * np.pi / length * np.mod(np.outer(left, right), length)
    return np.cos(angles), np.sin(angles)


def dft4(re, im):
    sr, si = re[0] + re[2], im[0] + im[2]
    dr, di = re[0] - re[2], im[0] - im[2]
    tr, ti = re[1] + re[3], im[1] + im[3]
    er, ei = re[1] - re[3], im[1] - im[3]
    return [sr + tr, dr + ei, sr - tr, dr - ei], [si + ti, di - er, si - ti, di + er]


def turn(re, im, step):
    step = step % POINTS
    if step == 0:
        return re, im
    if step == POINTS // 4:
        return im, -re
    c = float(np.cos(2.0 * np.pi * step / POINTS))
    s = float(np.sin(2.0 * np.pi * step / POINTS))
    if step == POINTS // 8:
        return (re + im) * c, (im - re) * c
    if step == 3 * POINTS // 8:
        return (im - re) * s, (re + im) * -s
    return re * c + im * s, im * c - re * s


def dft16(re, im):
    mid_re = [[None] * 4 for _ in range(4)]
    mid_im = [[None] * 4 for _ in range(4)]
    for n in range(4):
        yr, yi = dft4([re[4 * p + n] for p in range(4)], [im[4 * p + n] for p in range(4)])
        for k in range(4):
            mid_re[k][n], mid_im[k][n] = turn(yr[k], yi[k], n * k)
    out_re, out_im = [None] * POINTS, [None] * POINTS
    for k in range(4):
        yr, yi = dft4(mid_re[k], mid_im[k])
        for m in range(4):
            out_re[k + 4 * m], out_im[k + 4 * m] = yr[m], yi[m]
    return out_re, out_im


def fetch(*pairs):
    copies = [pltpu.make_async_copy(source, target, sem) for source, target, sem in pairs]
    for copy in copies:
        copy.start()
    return copies


def dot(a, b):
    return jnp.dot(a, b, preferred_element_type=f32)


def prepare_kernel(n_half, x_ref, y_ref):
    height, quarter = x_ref.shape
    rows_each = height // POINTS
    cols_each = quarter // POINTS
    share = height // n_half
    place = lax.broadcasted_iota(jnp.int32, (height, height), 0)
    source = lax.broadcasted_iota(jnp.int32, (height, height), 1)
    wanted = (place % rows_each) * POINTS + place // rows_each
    pick_rows = jnp.where(source == wanted, 1.0, 0.0).astype(bf16)
    ordered = dot(pick_rows, x_ref[...]).astype(bf16)
    place = lax.broadcasted_iota(jnp.int32, (quarter, quarter), 0)
    source = lax.broadcasted_iota(jnp.int32, (quarter, quarter), 1)
    wanted = (place % cols_each) * POINTS + place // cols_each
    pick_cols = jnp.where(source == wanted, 1.0, 0.0).astype(bf16)
    turned = lax.dot_general(
        pick_cols, ordered, (((1,), (1,)), ((), ())), preferred_element_type=f32
    ).astype(bf16)
    for j in range(n_half):
        for c in range(POINTS):
            y_ref[j, c] = turned[c * cols_each:(c + 1) * cols_each, j * share:(j + 1) * share]


def rows_kernel(n_rows, n_half, y_ref, w_hbm, t_hbm, z_ref, re_ref, im_ref, w_ref, t_ref, sems):
    copies = fetch((w_hbm, w_ref, sems.at[0]), (t_hbm, t_ref, sems.at[1]))
    share = y_ref.shape[3]
    span = z_ref.shape[2]
    half = LANES // 2
    lane = lax.broadcasted_iota(jnp.int32, (16, LANES), 1)

    for copy in copies:
        copy.wait()

    def first(g, carry):
        blocks = [
            jnp.concatenate([y_ref[j, g * GROUP + k] for j in range(n_half)], axis=0)
            for k in range(GROUP)
        ]
        block = jnp.concatenate(blocks, axis=1).T
        both = dot(block, w_ref[0]) + dot(block, w_ref[1])
        for k in range(GROUP):
            c = g * GROUP + k
            part = both[k * share:(k + 1) * share]
            re, im = part[:, :BOX], part[:, BOX:]
            tc, ts = t_ref[0, c], t_ref[1, c]
            re_ref[c] = re * tc + im * ts
            im_ref[c] = im * tc - re * ts
        return carry

    lax.fori_loop(0, POINTS // GROUP, first, 0)
    tiles = span // 16

    def second(t, carry):
        m = t // tiles
        at = pl.multiple_of((t % tiles) * 16, 16)
        row = pl.multiple_of(t * 16, 16)
        for h in range(BOX // LANES):
            lanes = pl.ds(h * LANES, LANES)
            re = [re_ref[c, pl.ds(row, 16), lanes] for c in range(POINTS)]
            im = [im_ref[c, pl.ds(row, 16), lanes] for c in range(POINTS)]
            re, im = dft16(re, im)
            for v in range(POINTS):
                slab = v * (BOX // LANES) + h
                to = (slab % n_rows) * n_half + slab // n_rows
                imag = pltpu.roll(im[v], half, 1)
                if 2 * slab < n_rows * n_half:
                    both = jnp.where(lane < half, re[v], imag)
                else:
                    both = jnp.where(lane < half, re[v], jnp.where(lane == half, im[v], imag))
                    both = jnp.where(lane == 0, pltpu.roll(re[v], half, 1), both)
                if slab == 0:
                    both = jnp.where(lane == half, pltpu.roll(re[POINTS // 2], half, 1), both)
                z_ref[to, m, pl.ds(at, 16), :] = both.astype(bf16)
        return carry

    lax.fori_loop(0, share // 16, second, 0)


def columns_kernel(n_rows, n_half, place_ref, z_ref, w_hbm, t_hbm, own_ref, far_ref, edge_ref,
                   re_ref, im_ref, mre_ref, mim_ref, mirror_ref, raw_ref, w_ref, t_ref, sems):
    copies = fetch((w_hbm, w_ref, sems.at[0]), (t_hbm, t_ref, sems.at[1]))
    kept = z_ref.shape[1]
    count = own_ref.shape[0]
    width = own_ref.shape[1]

    for copy in copies:
        copy.wait()

    def first(g, carry):
        blocks = []
        for k in range(GROUP):
            r = g * GROUP + k
            j, m = r // kept, r % kept
            blocks.append(
                jnp.concatenate([z_ref[i * n_half + j, m] for i in range(n_rows)], axis=0)
            )
        block = jnp.concatenate(blocks, axis=1).T
        product = dot(block, w_ref[0]) + dot(block, w_ref[1])
        for k in range(GROUP):
            r = g * GROUP + k
            both = product[2 * count * k:2 * count * (k + 1)]
            a, b = both[:count, :BOX], both[count:, :BOX]
            c, d = both[:count, BOX:], both[count:, BOX:]
            tc, ts = t_ref[0, r], t_ref[1, r]
            re, im = a - d, b + c
            re_ref[r] = re * tc + im * ts
            im_ref[r] = im * tc - re * ts
            tc, ts = t_ref[2, r], t_ref[3, r]
            re, im = a + d, b - c
            mre_ref[r] = re * tc + im * ts
            mim_ref[r] = im * tc - re * ts
        return carry

    lax.fori_loop(0, POINTS // GROUP, first, 0)

    def tile(t, raw):
        row = pl.multiple_of(t * 8, 8)
        for h in range(BOX // LANES):
            lanes = pl.ds(h * LANES, LANES)
            re = [re_ref[c, pl.ds(row, 8), lanes] for c in range(POINTS)]
            im = [im_ref[c, pl.ds(row, 8), lanes] for c in range(POINTS)]
            re, im = dft16(re, im)
            for u in range(POINTS):
                to = pl.ds(u * BOX + h * LANES, LANES)
                if raw:
                    raw_ref[0, :, to], raw_ref[1, :, to] = re[u], im[u]
                else:
                    own_ref[pl.ds(row, 8), to] = re[u] * re[u] + im[u] * im[u]
            re = [mre_ref[c, pl.ds(row, 8), lanes] for c in range(POINTS)]
            im = [mim_ref[c, pl.ds(row, 8), lanes] for c in range(POINTS)]
            re, im = dft16(re, im)
            for u in range(POINTS):
                to = pl.ds((POINTS - 1 - u) * BOX + h * LANES, LANES)
                if raw:
                    raw_ref[2, :, to], raw_ref[3, :, to] = re[u], im[u]
                else:
                    mirror_ref[pl.ds(row, 8), to] = re[u] * re[u] + im[u] * im[u]

    def second(t, carry):
        tile(t, False)
        return carry

    lax.fori_loop(0, count // 8, second, 0)
    tile(0, True)
    origin = place_ref[0] == 0
    for k in range(width // LANES):
        to = pl.ds(k * LANES, LANES)
        re, im, mre, mim = (raw_ref[n, 0:1, to] for n in range(4))
        even = 0.25 * ((re + mre) * (re + mre) + (im - mim) * (im - mim))
        odd = 0.25 * ((re - mre) * (re - mre) + (im + mim) * (im + mim))
        own_ref[0:1, to] = jnp.where(origin, even, own_ref[0:1, to])
        edge_ref[k:k + 1, :] = jnp.where(origin, odd, mirror_ref[0:1, to])
    place = lax.broadcasted_iota(jnp.int32, (count, count), 0)
    source = lax.broadcasted_iota(jnp.int32, (count, count), 1)
    flip = jnp.where((place + source) % count == 0, 1.0, 0.0).astype(bf16)
    for k in range(POINTS):
        to = pl.ds(k * BOX, BOX)
        far_ref[:, to] = dot(flip, mirror_ref[:, to].astype(bf16)).astype(bf16)


def power_kernel(place_ref, own_ref, far_ref, edge_ref, o_ref):
    count, width = own_ref.shape
    upper = place_ref[0] != 0
    o_ref[pl.ds(0, count), :] = own_ref[...]
    o_ref[pl.ds(count, count), :] = far_ref[...].astype(f32)
    for k in range(width // LANES):
        to = pl.ds(k * LANES, LANES)
        o_ref[0:1, to] = jnp.where(upper, edge_ref[k:k + 1, :], own_ref[0:1, to])
        o_ref[count:count + 1, to] = jnp.where(upper, own_ref[0:1, to], o_ref[count:count + 1, to])


def pieces_kernel(at_ref, x_ref, low_ref, x2_ref, low2_ref, own_ref, sent_ref, ext_ref):
    height, quarter = x_ref.shape
    tall, wide = height // BOX, quarter // BOX
    slots = own_ref.shape[0]
    chunk = 64
    mine = at_ref[4 * slots]
    ext_ref[mine, pl.ds(0, height), :] = x_ref[...]
    ext_ref[mine, pl.ds(height, BOX), :] = low_ref[...]
    ext_ref[1 - mine, pl.ds(0, height), :] = x2_ref[...]
    ext_ref[1 - mine, pl.ds(height, BOX), :] = low2_ref[...]

    def one(o_ref, first_slot, s):
        slot = first_slot + s
        top, left = at_ref[2 * slot], at_ref[2 * slot + 1]
        tile_row = jnp.clip(top >> 8, 0, tall - 1)
        tile_col = left >> 8
        row_cut, col_cut = top & (BOX - 1), left & (BOX - 1)
        here = jnp.logical_and(tile_col >= 0, tile_col < 2 * wide).astype(f32)
        after = jnp.logical_and(tile_col >= -1, tile_col < 2 * wide - 1).astype(f32)
        tile_a = jnp.clip(tile_col, 0, 2 * wide - 1)
        tile_b = jnp.clip(tile_col + 1, 0, 2 * wide - 1)
        side_a, side_b = tile_a // wide, tile_b // wide
        col_a = pl.multiple_of((tile_a % wide) * BOX, BOX)
        col_b = pl.multiple_of((tile_b % wide) * BOX, BOX)
        right = lax.broadcasted_iota(jnp.int32, (chunk, BOX), 1) >= col_cut
        rows = lax.broadcasted_iota(jnp.int32, (chunk, BOX), 0)
        for k in range(BOX // chunk):
            upper = pl.multiple_of(tile_row * BOX + k * chunk, chunk)
            lower = pl.multiple_of(tile_row * BOX + BOX + k * chunk, chunk)

            def across(first_row):
                a = ext_ref[side_a, pl.ds(first_row, chunk), pl.ds(col_a, BOX)].astype(f32) * here
                b = ext_ref[side_b, pl.ds(first_row, chunk), pl.ds(col_b, BOX)].astype(f32) * after
                return jnp.where(right, a, b)

            whole = jnp.where(rows + k * chunk >= row_cut, across(upper), across(lower))
            o_ref[s, pl.ds(k * chunk, chunk), :] = whole.astype(bf16)

    def both(s, carry):
        one(own_ref, 0, s)
        one(sent_ref, slots, s)
        return carry

    lax.fori_loop(0, slots, both, 0)


def spectra_kernel(n_planes, n_half, at_ref, p_ref, q_ref, w_hbm, c_hbm, *refs):
    members = len(refs) - 5
    o_refs, (w_ref, c_ref, w2_ref, c2_ref, sems) = refs[:members], refs[members:]
    copies = fetch((w_hbm, w_ref, sems.at[0]), (c_hbm, c_ref, sems.at[1]))
    slots = q_ref.shape[0]
    wide = 2 * BOX
    band = wide // n_half
    tall = o_refs[0].shape[2]
    beside = members // n_half
    plane, side, column = (at_ref[2 * slots + n] for n in range(3))
    for copy in copies:
        copy.wait()
    for part in range(2):
        for k in range(n_planes):
            for i in range(beside):
                first = (lax.rem(plane + k, n_planes) * beside + (side ^ i)) * tall
                rows = c_ref[part, pl.ds(pl.multiple_of(first, tall), tall), :]
                c2_ref[part, pl.ds((k * beside + i) * tall, tall), :] = rows
        for half in range(2):
            for j in range(n_half):
                first = pl.multiple_of((column ^ j) * band + half * wide, band)
                w2_ref[part, :, pl.ds(j * band + half * wide, band)] = w_ref[part, :, pl.ds(first, band)]

    def one(s, carry):
        box = p_ref[s].astype(f32) + q_ref[s].astype(f32)
        box = pltpu.roll(box, at_ref[2 * s], 0)
        box = pltpu.roll(box, at_ref[2 * s + 1], 1).astype(bf16)
        inner = dot(box, w2_ref[0]) + dot(box, w2_ref[1])
        high = inner.astype(bf16)
        low = (inner - high.astype(f32)).astype(bf16)
        high = jnp.concatenate([high[:, :wide], high[:, wide:]], axis=0)
        low = jnp.concatenate([low[:, :wide], low[:, wide:]], axis=0)
        outer = dot(c2_ref[0], high) + dot(c2_ref[0], low) + dot(c2_ref[1], high)
        outer = outer.astype(bf16)
        for k in range(n_planes):
            for i in range(beside):
                row = (k * beside + i) * tall
                for j in range(n_half):
                    o_refs[i * n_half + j][k, s] = outer[row:row + tall, j * band:(j + 1) * band]
        return carry

    lax.fori_loop(0, slots, one, 0, unroll=2)


def gather_kernel(members, *refs):
    sides, outs = refs[:members], refs[members:]
    slots = sides[0].shape[1]
    for k, out_ref in enumerate(outs):
        for m, side_ref in enumerate(sides):
            out_ref[pl.ds(m * slots, slots)] = side_ref[k]


def means_kernel(label_ref, live_ref, divisor_ref, *refs):
    count = (len(refs) - 1) // 2
    f_refs, o_ref, sum_refs = refs[:count], refs[count], refs[count + 1:]
    here = f_refs[0].shape[0]
    half = f_refs[0].shape[2] // 2
    for sum_ref in sum_refs:
        sum_ref[...] = jnp.zeros_like(sum_ref)

    def add(g, carry):
        for n, (f_ref, sum_ref) in enumerate(zip(f_refs, sum_refs)):
            k = label_ref[n * here + g]
            live = live_ref[n * here + g].astype(f32)
            sum_ref[k] = sum_ref[k] + f_ref[g].astype(f32) * live
        return carry

    lax.fori_loop(0, here, add, 0, unroll=4)

    def finish(k, carry):
        mean = sum_refs[0][k]
        for sum_ref in sum_refs[1:]:
            mean = mean + sum_ref[k]
        mean = mean / divisor_ref[k]
        o_ref[k, 0] = mean[:, :half]
        o_ref[k, 1] = mean[:, half:]
        return carry

    lax.fori_loop(0, o_ref.shape[0], finish, 0, unroll=5)


def swapped(block, axis, bit):
    route = [(i, i ^ bit) for i in range(lax.axis_size(axis))]
    return lax.ppermute(block, axis, route)


def fast_device(micrograph, box_tops, box_live, box_class, box_shift):
    n_rows = lax.axis_size("rows")
    n_half = lax.axis_size("half")
    everyone = ("rows", "half")
    total = n_rows * n_half
    height, quarter = micrograph.shape
    width = quarter * n_half
    row_index = lax.axis_index("rows")
    half_index = lax.axis_index("half")
    kept = POINTS // n_half
    span = height // POINTS
    slab = quarter // n_rows
    slots = box_tops.shape[2]
    shape = jax.ShapeDtypeStruct

    below = passed_along(micrograph[:BOX], "rows", -1)
    micrograph2 = swapped(micrograph, "half", 1)

    points = np.arange(BOX)
    cos_box, sin_box = waves(points, points, BOX)

    def table(values):
        return pltpu.with_memory_space_constraint(jnp.asarray(values), pltpu.HBM)

    first = np.stack(halves(np.concatenate([cos_box, -sin_box], axis=1)))
    tc, ts = waves(np.arange(POINTS), points, width)
    mc, ms = waves(np.arange(POINTS), BOX - points, width)
    turns = np.stack([tc, ts]).astype(np.float32)[:, :, None]
    turns_both = (np.stack([tc, ts, mc, ms]) / width).astype(np.float32)[:, :, None]

    def fetched(*tables):
        return [pltpu.VMEM(t.shape, t.dtype) for t in tables] + [pltpu.SemaphoreType.DMA((len(tables),))]

    ready = call(
        functools.partial(prepare_kernel, n_half),
        shape((n_half, POINTS, quarter // POINTS, height // n_half), bf16),
        [micrograph], [VMEM],
        flops=2 * height * quarter * (height + quarter),
    )
    ready = lax.all_to_all(ready, "half", 0, 0, tiled=True)
    below2 = swapped(below, "half", 1)
    mixed = call(
        functools.partial(rows_kernel, n_rows, n_half),
        shape((total, kept, span, slab), bf16),
        [ready, table(first), table(turns)], [VMEM, HBM, HBM],
        scratch=[pltpu.VMEM((POINTS, height // n_half, BOX), f32)] * 2 + fetched(first, turns),
        flops=4 * height * quarter * 2 * BOX,
    )
    mixed = lax.all_to_all(mixed, everyone, 0, 0, tiled=True)

    core = half_index % 2
    corner = jnp.stack([row_index * height, (half_index - core) * quarter])
    band_tops = box_tops[row_index]
    at = jnp.stack([band_tops[half_index], band_tops[half_index ^ 2]]) - corner
    at = jnp.concatenate([at.reshape(-1), core.reshape(1)])
    pieces, sent = call(
        pieces_kernel,
        (shape((slots, BOX, BOX), bf16),) * 2,
        [at, micrograph, below, micrograph2, below2], [SMEM] + [VMEM] * 4,
        scratch=[pltpu.VMEM((2, height + BOX, quarter), bf16)],
        flops=20 * slots * BOX * BOX,
    )
    across = swapped(sent, "half", 2)
    part = BOX // n_half

    def by_part(a, b):
        a = a.reshape(-1, n_half, 1, part)
        b = b.reshape(-1, n_half, 1, part)
        return np.concatenate([a, b], axis=2).reshape(-1, 2 * BOX)

    plain = by_part(cos_box, -sin_box)
    crossed = by_part(-sin_box, -cos_box)
    inner = np.stack(halves(np.concatenate([plain, crossed], axis=1) / BOX))
    outer = np.stack(halves(np.concatenate([cos_box, sin_box], axis=1)))
    my_tops = box_tops[row_index, half_index]
    rolls = jnp.mod(box_shift.reshape(slots, 2) - my_tops, BOX).reshape(-1)
    n_planes = n_rows // 2
    members = total // n_planes
    plane = row_index // 2
    member = (row_index % 2) * n_half + half_index
    spot = jnp.stack([plane, row_index % 2, half_index])
    spectra = call(
        functools.partial(spectra_kernel, n_planes, n_half),
        (shape((n_planes, slots, BOX // n_rows, 2 * part), bf16),) * members,
        [jnp.concatenate([rolls, spot]), pieces, across, table(inner), table(outer)],
        [SMEM, VMEM, VMEM, HBM, HBM],
        scratch=[pltpu.VMEM(t.shape, t.dtype) for t in (inner, outer)] + fetched(inner, outer),
        flops=slots * BOX * BOX * 4 * BOX * 10,
    )
    sides = [spectra[0]]
    for m in range(1, members):
        route = [(d, d - d % members + (d % members ^ m)) for d in range(total)]
        sides.append(lax.ppermute(spectra[m], everyone, route))
    gathered = call(
        functools.partial(gather_kernel, members),
        (shape((members * slots, BOX // n_rows, 2 * part), bf16),) * n_planes,
        sides, [VMEM] * members,
        flops=total * slots * BOX * BOX // 8,
    )

    arrived = [gathered[0]]
    for k in range(1, n_planes):
        route = [(d, (d + k * members) % total) for d in range(total)]
        arrived.append(lax.ppermute(gathered[k], everyone, route))

    def source_order(values):
        values = values.reshape(n_planes, members, slots)
        ids = jnp.arange(max(n_planes, members), dtype=jnp.int32)
        values = values[jnp.mod(plane - ids[:n_planes], n_planes)]
        return values[:, member ^ ids[:members]].reshape(-1)

    half = slab // 2
    place = half_index * n_rows + row_index
    own, far, edge = call(
        functools.partial(columns_kernel, n_rows, n_half),
        (shape((half, width), f32), shape((half, width), bf16), shape((width // LANES, LANES), f32)),
        [place.reshape(1), mixed, table(first), table(turns_both)], [SMEM, VMEM, HBM, HBM],
        scratch=[pltpu.VMEM((POINTS, half, BOX), f32)] * 4
        + [pltpu.VMEM((half, width), f32), pltpu.VMEM((4, 8, width), f32)]
        + fetched(first, turns_both),
        flops=8 * slab * width * 2 * BOX,
    )
    far = lax.ppermute(far, everyone, [(d, total - 1 - d) for d in range(total)])
    seats = [(p % n_rows) * n_half + p // n_rows for p in range(total)]
    route = [(p, total - p) for p in range(1, total // 2)] + [(0, total // 2)]
    edge = lax.ppermute(edge, everyone, [(seats[a], seats[b]) for a, b in route])
    power = call(
        power_kernel,
        shape((slab, width), f32),
        [(2 * place >= total).astype(jnp.int32).reshape(1), own, far, edge], [SMEM] + [VMEM] * 3,
        flops=slab * width,
    )[None]
    labels, lives = box_class.reshape(-1), box_live.reshape(-1)
    matches = labels[None, :] == jnp.arange(CLASSES, dtype=jnp.int32)[:, None]
    counts = jnp.sum(jnp.where(matches, lives[None, :], 0), axis=1)
    divisor = jnp.maximum(counts, 1).astype(f32)
    labels_here, lives_here = source_order(box_class), source_order(box_live)
    class_means = call(
        means_kernel,
        shape((CLASSES, 2, BOX // n_rows, part), f32),
        [labels_here, lives_here, divisor, *arrived], [SMEM] * 3 + [VMEM] * len(arrived),
        scratch=[pltpu.VMEM((CLASSES, BOX // n_rows, 2 * part), f32)] * n_planes,
        flops=4 * total * slots * BOX * BOX,
    )
    return (power, class_means)


def fits(mesh, micrograph):
    height, quarter = micrograph.shape
    n_rows, n_half = mesh.shape["rows"], mesh.shape["half"]
    return (
        height * n_rows == POINTS * BOX
        and quarter * n_half == POINTS * BOX
        and n_half == 4
        and height % BOX == 0
        and quarter % BOX == 0
        and height // n_half == LANES
        and quarter // n_rows == LANES
        and BOX // n_rows % 16 == 0
        and 2 * BOX // n_half == LANES
        and n_rows == 8
    )


def solution(mesh):
    in_specs = (P("rows", "half"), P(), P(), P(), P("rows", "half", None, None))
    out_specs = (P("half", "rows", None), P(None, None, "rows", "half"))

    def per_device(micrograph, *boxes):
        device = fast_device if fits(mesh, micrograph) else general_device
        return device(micrograph, *boxes)

    return jax.shard_map(
        per_device, mesh=mesh, in_specs=in_specs, out_specs=out_specs, check_vma=False
    )
```

```python
import functools

import numpy as np

import jax
import jax.numpy as jnp
from jax import lax
from jax.experimental import pallas as pl
from jax.experimental.pallas import tpu as pltpu
from jax.sharding import PartitionSpec as P


BOX = 256
CLASSES = 50
RADIX = 64
LANES = 128
POINTS = 16

highest = lax.Precision.HIGHEST


def passed_along(block, axis, distance):
    devices = range(lax.axis_size(axis))
    route = [(i - distance, i) for i in devices if i - distance in devices]
    return lax.ppermute(block, axis, route)


def phases(left_index, right_index, length):
    rotations = jnp.mod(left_index[:, None] * right_index[None, :], length)
    angles = 2.0 * jnp.pi / length * rotations.astype(jnp.float32)
    return (jnp.cos(angles), jnp.sin(angles))


def product(pattern, left_side, matrix):
    return jnp.einsum(pattern, left_side, matrix, precision=highest)


def four_step(real_part, imag_part, first_index, how_many, rows_last):
    height = real_part.shape[0]
    length = real_part.shape[1]
    outer_size = RADIX
    inner_size = length // outer_size
    real_part = real_part.reshape(height, outer_size, inner_size)
    spread = jnp.arange(outer_size, dtype=jnp.int32)
    across = jnp.arange(inner_size, dtype=jnp.int32)
    cos_one, sin_one = phases(spread, spread, outer_size)
    section_real = product("mab,ka->mkb", real_part, cos_one)
    section_imag = -product("mab,ka->mkb", real_part, sin_one)
    if imag_part is not None:
        imag_part = imag_part.reshape(height, outer_size, inner_size)
        section_real = section_real + product("mab,ka->mkb", imag_part, sin_one)
        section_imag = section_imag + product("mab,ka->mkb", imag_part, cos_one)
    twist_cos, twist_sin = phases(spread, across, length)
    turned_real = section_real * twist_cos + section_imag * twist_sin
    turned_imag = section_imag * twist_cos - section_real * twist_sin
    wanted = first_index + jnp.arange(how_many, dtype=jnp.int32)
    cos_two, sin_two = phases(wanted, across, inner_size)
    pattern = "mkb,tb->tkm" if rows_last else "mkb,tb->mtk"
    out_real = product(pattern, turned_real, cos_two) + product(pattern, turned_imag, sin_two)
    out_imag = product(pattern, turned_imag, cos_two) - product(pattern, turned_real, sin_two)
    return (out_real, out_imag)


def general_device(micrograph, box_tops, box_live, box_class, box_shift):
    row_index = lax.axis_index("rows")
    half_index = lax.axis_index("half")
    band_rows = lax.all_gather(micrograph, "half", axis=1, tiled=True)
    height = band_rows.shape[0]
    full_width = band_rows.shape[1]
    quarter = full_width // lax.axis_size("half")
    per_block = quarter // RADIX
    image_rows = band_rows.astype(jnp.float32)
    part_real, part_imag = four_step(image_rows, None, half_index * per_block, per_block, True)
    partial_value = jnp.stack(
        [part_real.reshape(quarter, height), part_imag.reshape(quarter, height)]
    )
    columns = lax.all_to_all(partial_value, "rows", split_axis=1, concat_axis=2, tiled=True)
    column_count = columns.shape[1]
    freq_real, freq_imag = four_step(columns[0], columns[1], 0, full_width // RADIX, False)
    power_out = (freq_real * freq_real + freq_imag * freq_imag).reshape(1, column_count, full_width)
    power_out = power_out / (full_width * full_width)
    local_tops = box_tops[row_index, half_index]
    start_rows = local_tops[:, 0] - row_index * height
    start_cols = local_tops[:, 1]
    reach_bands = (BOX + height - 2) // height

    def cut_columns(source, corner):
        return lax.dynamic_slice_in_dim(source, corner, BOX, 1)

    pieces = [jax.vmap(cut_columns, (None, 0))(band_rows, start_cols)]
    for offset in range(1, reach_bands + 1):
        target = jnp.maximum(row_index - offset, 0)
        their_cols = box_tops[target, half_index][:, 1]
        outgoing = jax.vmap(cut_columns, (None, 0))(band_rows, their_cols)
        pieces.append(passed_along(outgoing, "rows", -offset))
    windows = jnp.concatenate(pieces, axis=1)
    particle_boxes = jax.vmap(
        lambda window, corner: lax.dynamic_slice_in_dim(window, corner, BOX, 0)
    )(windows, start_rows)
    frequency = jnp.arange(BOX, dtype=jnp.int32)
    cos_box, sin_box = phases(frequency, frequency, BOX)
    local_offsets = box_shift.reshape(-1, 2)

    def spectrum(member):
        particle, offsets_pair = member
        values = particle.astype(jnp.float32)
        inner_real = jnp.dot(values, cos_box, precision=highest)
        inner_imag = -jnp.dot(values, sin_box, precision=highest)
        outer_real = (
            jnp.dot(cos_box, inner_real, precision=highest)
            + jnp.dot(sin_box, inner_imag, precision=highest)
        ) / BOX
        outer_imag = (
            jnp.dot(cos_box, inner_imag, precision=highest)
            - jnp.dot(sin_box, inner_real, precision=highest)
        ) / BOX
        rotations = jnp.mod(
            frequency[:, None] * offsets_pair[0] + frequency[None, :] * offsets_pair[1], BOX
        )
        angles = 2.0 * jnp.pi / BOX * rotations.astype(jnp.float32)
        ramp_cos = jnp.cos(angles)
        ramp_sin = jnp.sin(angles)
        shifted_real = outer_real * ramp_cos + outer_imag * ramp_sin
        shifted_imag = outer_imag * ramp_cos - outer_real * ramp_sin
        return jnp.stack([shifted_real, shifted_imag]).astype(jnp.bfloat16)

    spectra = lax.map(spectrum, (particle_boxes, local_offsets))
    classes_all = jnp.arange(CLASSES, dtype=jnp.int32)
    all_labels = box_class.reshape(-1)
    all_live = box_live.reshape(-1)
    counts = jnp.sum(
        (all_labels[None, :] == classes_all[:, None]).astype(jnp.int32) * all_live[None, :], axis=1
    )
    arrived = lax.all_to_all(spectra, "rows", split_axis=2, concat_axis=0, tiled=True)
    chosen_labels = box_class[:, half_index].reshape(-1)
    chosen_live = box_live[:, half_index].reshape(-1)
    weights = (
        (chosen_labels[None, :] == classes_all[:, None]).astype(jnp.int32) * chosen_live[None, :]
    ).astype(jnp.bfloat16)
    flat_spectra = arrived.reshape(arrived.shape[0], -1)
    partial_sums = jnp.dot(weights, flat_spectra, preferred_element_type=jnp.float32)
    partial_sums = partial_sums.reshape((CLASSES,) + arrived.shape[1:])
    class_sums = lax.psum_scatter(partial_sums, "half", scatter_dimension=3, tiled=True)
    divisor = jnp.maximum(counts, 1).astype(jnp.float32)
    class_means = class_sums / divisor[:, None, None, None]
    return (power_out, class_means)


GROUP = 4
SUMS = 4
f32 = jnp.float32
bf16 = jnp.bfloat16
VMEM = pl.BlockSpec(memory_space=pltpu.VMEM)
SMEM = pl.BlockSpec(memory_space=pltpu.SMEM)
HBM = pl.BlockSpec(memory_space=pltpu.HBM)

def call(kernel, out, operands, specs, scratch=(), flops=0):
    made = out if isinstance(out, tuple) else (out,)
    moved = sum(a.size * a.dtype.itemsize for a in (*operands, *made))
    return pl.pallas_call(
        kernel,
        out_shape=out,
        in_specs=specs,
        out_specs=(VMEM,) * len(out) if isinstance(out, tuple) else VMEM,
        scratch_shapes=list(scratch),
        compiler_params=pltpu.CompilerParams(vmem_limit_bytes=48 * 1024 * 1024),
        cost_estimate=pl.CostEstimate(flops=flops, bytes_accessed=moved, transcendentals=0),
    )(*operands)

def halves(table):
    high = table.astype(bf16)
    low = (table - high.astype(np.float64)).astype(bf16)
    return high, low

def waves(left, right, length):
    angles = 2.0 * np.pi / length * np.mod(np.outer(left, right), length)
    return np.cos(angles), np.sin(angles)

def dft4(re, im):
    sr, si = re[0] + re[2], im[0] + im[2]
    dr, di = re[0] - re[2], im[0] - im[2]
    tr, ti = re[1] + re[3], im[1] + im[3]
    er, ei = re[1] - re[3], im[1] - im[3]
    return [sr + tr, dr + ei, sr - tr, dr - ei], [si + ti, di - er, si - ti, di + er]

def turn(re, im, step):
    step = step % POINTS
    if step == 0:
        return re, im
    if step == POINTS // 4:
        return im, -re
    c = float(np.cos(2.0 * np.pi * step / POINTS))
    s = float(np.sin(2.0 * np.pi * step / POINTS))
    if step == POINTS // 8:
        return (re + im) * c, (im - re) * c
    if step == 3 * POINTS // 8:
        return (im - re) * s, (re + im) * -s
    return re * c + im * s, im * c - re * s

def dft16(re, im):
    mid_re = [[None] * 4 for _ in range(4)]
    mid_im = [[None] * 4 for _ in range(4)]
    for n in range(4):
        yr, yi = dft4([re[4 * p + n] for p in range(4)], [im[4 * p + n] for p in range(4)])
        for k in range(4):
            mid_re[k][n], mid_im[k][n] = turn(yr[k], yi[k], n * k)
    out_re, out_im = [None] * POINTS, [None] * POINTS
    for k in range(4):
        yr, yi = dft4(mid_re[k], mid_im[k])
        for m in range(4):
            out_re[k + 4 * m], out_im[k + 4 * m] = yr[m], yi[m]
    return out_re, out_im

def fetch(*pairs):
    copies = [pltpu.make_async_copy(source, target, sem) for source, target, sem in pairs]
    for copy in copies:
        copy.start()
    return copies

def dot(a, b):
    return jnp.dot(a, b, preferred_element_type=f32)

def one_hot(size, wanted):
    place = lax.broadcasted_iota(jnp.int32, (size, size), 0)
    source = lax.broadcasted_iota(jnp.int32, (size, size), 1)
    return jnp.where(source == wanted(place), 1.0, 0.0).astype(bf16)

def prepare_kernel(n_half, x_ref, y_ref):
    height, quarter = x_ref.shape
    each = BOX // POINTS
    share = height // n_half
    rows_each = height // POINTS
    pick_rows = one_hot(height, lambda p: (p % rows_each) * POINTS + p // rows_each)
    pick_cols = one_hot(BOX, lambda p: (p % each) * POINTS + p // each)
    for k in range(quarter // BOX):
        ordered = dot(pick_rows, x_ref[:, k * BOX:(k + 1) * BOX]).astype(bf16)
        turned = lax.dot_general(
            pick_cols, ordered, (((1,), (1,)), ((), ())), preferred_element_type=f32
        ).astype(bf16)
        for j in range(n_half):
            for c in range(POINTS):
                y_ref[j, c, k * each:(k + 1) * each] = (
                    turned[c * each:(c + 1) * each, j * share:(j + 1) * share]
                )

def rows_kernel(n_rows, n_half, y_ref, w_hbm, t_hbm, z_ref, re_ref, im_ref, turned_ref, w_ref, t_ref, sems):
    copies = fetch((w_hbm, w_ref, sems.at[0]), (t_hbm, t_ref, sems.at[1]))
    share = y_ref.shape[3]
    span = z_ref.shape[2]
    half = LANES // 2
    lane = lax.broadcasted_iota(jnp.int32, (16, LANES), 1)

    def turn_blocks(g, carry):
        blocks = [
            jnp.concatenate([y_ref[j, g * GROUP + k] for j in range(n_half)], axis=0)
            for k in range(GROUP)
        ]
        turned_ref[g] = jnp.concatenate(blocks, axis=1).T
        return carry

    lax.fori_loop(0, POINTS // GROUP, turn_blocks, 0)
    for copy in copies:
        copy.wait()

    def first(g, carry):
        block = turned_ref[g]
        both = dot(block, w_ref[0]) + dot(block, w_ref[1])
        for k in range(GROUP):
            c = g * GROUP + k
            part = both[k * share:(k + 1) * share]
            re, im = part[:, :BOX], part[:, BOX:]
            tc, ts = t_ref[0, c], t_ref[1, c]
            re_ref[c] = re * tc + im * ts
            im_ref[c] = im * tc - re * ts
        return carry

    lax.fori_loop(0, POINTS // GROUP, first, 0)
    tiles = span // 16

    def second(t, carry):
        m = t // tiles
        at = pl.multiple_of((t % tiles) * 16, 16)
        row = pl.multiple_of(t * 16, 16)
        for h in range(BOX // LANES):
            lanes = pl.ds(h * LANES, LANES)
            re = [re_ref[c, pl.ds(row, 16), lanes] for c in range(POINTS)]
            im = [im_ref[c, pl.ds(row, 16), lanes] for c in range(POINTS)]
            re, im = dft16(re, im)
            for v in range(POINTS):
                slab = v * (BOX // LANES) + h
                to = (slab % n_rows) * n_half + slab // n_rows
                imag = pltpu.roll(im[v], half, 1)
                if 2 * slab < n_rows * n_half:
                    both = jnp.where(lane < half, re[v], imag)
                else:
                    both = jnp.where(lane < half, re[v], jnp.where(lane == half, im[v], imag))
                    both = jnp.where(lane == 0, pltpu.roll(re[v], half, 1), both)
                if slab == 0:
                    both = jnp.where(lane == half, pltpu.roll(re[POINTS // 2], half, 1), both)
                z_ref[to, m, pl.ds(at, 16), :] = both.astype(bf16)
        return carry

    lax.fori_loop(0, share // 16, second, 0)

def columns_kernel(n_rows, n_half, place_ref, z_ref, w_hbm, t_hbm, own_ref, far_ref, edge_ref,
                   re_ref, im_ref, mre_ref, mim_ref, mirror_ref, raw_ref, turned_ref, w_ref, t_ref, sems):
    copies = fetch((w_hbm, w_ref, sems.at[0]), (t_hbm, t_ref, sems.at[1]))
    kept = z_ref.shape[1]
    count = own_ref.shape[0]
    width = own_ref.shape[1]

    def turn_blocks(g, carry):
        blocks = []
        for k in range(GROUP):
            r = g * GROUP + k
            j, m = r // kept, r % kept
            blocks.append(
                jnp.concatenate([z_ref[i * n_half + j, m] for i in range(n_rows)], axis=0)
            )
        turned_ref[g] = jnp.concatenate(blocks, axis=1).T
        return carry

    lax.fori_loop(0, POINTS // GROUP, turn_blocks, 0)
    for copy in copies:
        copy.wait()

    def first(g, carry):
        block = turned_ref[g]
        product = dot(block, w_ref[0]) + dot(block, w_ref[1])
        for k in range(GROUP):
            r = g * GROUP + k
            both = product[2 * count * k:2 * count * (k + 1)]
            a, b = both[:count, :BOX], both[count:, :BOX]
            c, d = both[:count, BOX:], both[count:, BOX:]
            tc, ts = t_ref[0, r], t_ref[1, r]
            re, im = a - d, b + c
            re_ref[r] = re * tc + im * ts
            im_ref[r] = im * tc - re * ts
            tc, ts = t_ref[2, r], t_ref[3, r]
            re, im = a + d, b - c
            mre_ref[r] = re * tc + im * ts
            mim_ref[r] = im * tc - re * ts
        return carry

    lax.fori_loop(0, POINTS // GROUP, first, 0)

    def tile(t, raw):
        row = pl.multiple_of(t * 8, 8)
        for h in range(BOX // LANES):
            lanes = pl.ds(h * LANES, LANES)
            re = [re_ref[c, pl.ds(row, 8), lanes] for c in range(POINTS)]
            im = [im_ref[c, pl.ds(row, 8), lanes] for c in range(POINTS)]
            re, im = dft16(re, im)
            for u in range(POINTS):
                to = pl.ds(u * BOX + h * LANES, LANES)
                if raw:
                    raw_ref[0, :, to], raw_ref[1, :, to] = re[u], im[u]
                else:
                    own_ref[pl.ds(row, 8), to] = re[u] * re[u] + im[u] * im[u]
            re = [mre_ref[c, pl.ds(row, 8), lanes] for c in range(POINTS)]
            im = [mim_ref[c, pl.ds(row, 8), lanes] for c in range(POINTS)]
            re, im = dft16(re, im)
            for u in range(POINTS):
                to = pl.ds((POINTS - 1 - u) * BOX + h * LANES, LANES)
                if raw:
                    raw_ref[2, :, to], raw_ref[3, :, to] = re[u], im[u]
                else:
                    mirror_ref[pl.ds(row, 8), to] = re[u] * re[u] + im[u] * im[u]

    def second(t, carry):
        tile(t, False)
        return carry

    lax.fori_loop(0, count // 8, second, 0)
    tile(0, True)
    origin = place_ref[0] == 0
    for k in range(width // LANES):
        to = pl.ds(k * LANES, LANES)
        re, im, mre, mim = (raw_ref[n, 0:1, to] for n in range(4))
        even = 0.25 * ((re + mre) * (re + mre) + (im - mim) * (im - mim))
        odd = 0.25 * ((re - mre) * (re - mre) + (im + mim) * (im + mim))
        own_ref[0:1, to] = jnp.where(origin, even, own_ref[0:1, to])
        edge_ref[k:k + 1, :] = jnp.where(origin, odd, mirror_ref[0:1, to])
    place = lax.broadcasted_iota(jnp.int32, (count, count), 0)
    source = lax.broadcasted_iota(jnp.int32, (count, count), 1)
    flip = jnp.where((place + source) % count == 0, 1.0, 0.0).astype(bf16)
    for k in range(POINTS):
        to = pl.ds(k * BOX, BOX)
        far_ref[:, to] = dot(flip, mirror_ref[:, to].astype(bf16)).astype(bf16)

def power_kernel(place_ref, own_ref, far_ref, edge_ref, o_ref):
    count, width = own_ref.shape
    upper = place_ref[0] != 0
    o_ref[pl.ds(0, count), :] = own_ref[...]
    o_ref[pl.ds(count, count), :] = far_ref[...].astype(f32)
    for k in range(width // LANES):
        to = pl.ds(k * LANES, LANES)
        o_ref[0:1, to] = jnp.where(upper, edge_ref[k:k + 1, :], own_ref[0:1, to])
        o_ref[count:count + 1, to] = jnp.where(upper, own_ref[0:1, to], o_ref[count:count + 1, to])

def pieces_kernel(at_ref, x_ref, low_ref, x2_ref, low2_ref, own_ref, sent_ref, ext_ref):
    height, quarter = x_ref.shape
    tall, wide = height // BOX, quarter // BOX
    slots = own_ref.shape[0]
    chunk = 64
    mine = at_ref[4 * slots]
    ext_ref[mine, pl.ds(0, height), :] = x_ref[...]
    ext_ref[mine, pl.ds(height, BOX), :] = low_ref[...]
    ext_ref[1 - mine, pl.ds(0, height), :] = x2_ref[...]
    ext_ref[1 - mine, pl.ds(height, BOX), :] = low2_ref[...]

    def one(o_ref, first_slot, s):
        slot = first_slot + s
        top, left = at_ref[2 * slot], at_ref[2 * slot + 1]
        tile_row = jnp.clip(top >> 8, 0, tall - 1)
        tile_col = left >> 8
        row_cut, col_cut = top & (BOX - 1), left & (BOX - 1)
        here = jnp.logical_and(tile_col >= 0, tile_col < 2 * wide).astype(f32)
        after = jnp.logical_and(tile_col >= -1, tile_col < 2 * wide - 1).astype(f32)
        tile_a = jnp.clip(tile_col, 0, 2 * wide - 1)
        tile_b = jnp.clip(tile_col + 1, 0, 2 * wide - 1)
        side_a, side_b = tile_a // wide, tile_b // wide
        col_a = pl.multiple_of((tile_a % wide) * BOX, BOX)
        col_b = pl.multiple_of((tile_b % wide) * BOX, BOX)
        right = lax.broadcasted_iota(jnp.int32, (chunk, BOX), 1) >= col_cut
        rows = lax.broadcasted_iota(jnp.int32, (chunk, BOX), 0)
        for k in range(BOX // chunk):
            upper = pl.multiple_of(tile_row * BOX + k * chunk, chunk)
            lower = pl.multiple_of(tile_row * BOX + BOX + k * chunk, chunk)

            def across(first_row):
                a = ext_ref[side_a, pl.ds(first_row, chunk), pl.ds(col_a, BOX)].astype(f32) * here
                b = ext_ref[side_b, pl.ds(first_row, chunk), pl.ds(col_b, BOX)].astype(f32) * after
                return jnp.where(right, a, b)

            whole = jnp.where(rows + k * chunk >= row_cut, across(upper), across(lower))
            o_ref[s, pl.ds(k * chunk, chunk), :] = whole.astype(bf16)

    def both(s, carry):
        one(own_ref, 0, s)
        one(sent_ref, slots, s)
        return carry

    lax.fori_loop(0, slots, both, 0)

def spectra_kernel(n_planes, n_half, at_ref, p_ref, q_ref, w_hbm, c_hbm, *refs):
    members = len(refs) - 5
    o_refs, (w_ref, c_ref, w2_ref, c2_ref, sems) = refs[:members], refs[members:]
    copies = fetch((w_hbm, w_ref, sems.at[0]), (c_hbm, c_ref, sems.at[1]))
    slots = q_ref.shape[0]
    wide = 2 * BOX
    band = wide // n_half
    tall = o_refs[0].shape[2]
    beside = members // n_half
    plane, side, column = (at_ref[2 * slots + n] for n in range(3))
    for copy in copies:
        copy.wait()
    for part in range(2):
        for k in range(n_planes):
            for i in range(beside):
                first = (lax.rem(plane + k, n_planes) * beside + (side ^ i)) * tall
                rows = c_ref[part, pl.ds(pl.multiple_of(first, tall), tall), :]
                c2_ref[part, pl.ds((k * beside + i) * tall, tall), :] = rows
        for half in range(2):
            for j in range(n_half):
                first = pl.multiple_of((column ^ j) * band + half * wide, band)
                w2_ref[part, :, pl.ds(j * band + half * wide, band)] = w_ref[part, :, pl.ds(first, band)]

    def one(s, carry):
        box = p_ref[s].astype(f32) + q_ref[s].astype(f32)
        box = pltpu.roll(box, at_ref[2 * s], 0)
        box = pltpu.roll(box, at_ref[2 * s + 1], 1).astype(bf16)
        inner = dot(box, w2_ref[0]) + dot(box, w2_ref[1])
        high = inner.astype(bf16)
        low = (inner - high.astype(f32)).astype(bf16)
        high = jnp.concatenate([high[:, :wide], high[:, wide:]], axis=0)
        low = jnp.concatenate([low[:, :wide], low[:, wide:]], axis=0)
        outer = dot(c2_ref[0], high) + dot(c2_ref[0], low) + dot(c2_ref[1], high)
        outer = outer.astype(bf16)
        for k in range(n_planes):
            for i in range(beside):
                row = (k * beside + i) * tall
                for j in range(n_half):
                    o_refs[i * n_half + j][k, s] = outer[row:row + tall, j * band:(j + 1) * band]
        return carry

    lax.fori_loop(0, slots, one, 0, unroll=2)

def gather_kernel(members, *refs):
    sides, outs = refs[:members], refs[members:]
    slots = sides[0].shape[1]
    for k, out_ref in enumerate(outs):
        for m, side_ref in enumerate(sides):
            out_ref[pl.ds(m * slots, slots)] = side_ref[k]

def means_kernel(label_ref, live_ref, divisor_ref, *refs):
    count = len(refs) - 1 - SUMS
    f_refs, o_ref, sum_refs = refs[:count], refs[count], refs[count + 1:]
    here = f_refs[0].shape[0]
    half = f_refs[0].shape[2] // 2
    for sum_ref in sum_refs:
        sum_ref[...] = jnp.zeros_like(sum_ref)

    def add(g, carry):
        for n, f_ref in enumerate(f_refs):
            sum_ref = sum_refs[n % SUMS]
            k = label_ref[n * here + g]
            live = live_ref[n * here + g].astype(f32)
            sum_ref[k] = sum_ref[k] + f_ref[g].astype(f32) * live
        return carry

    lax.fori_loop(0, here, add, 0, unroll=4)

    def finish(k, carry):
        mean = sum_refs[0][k]
        for sum_ref in sum_refs[1:]:
            mean = mean + sum_ref[k]
        mean = mean / divisor_ref[k]
        o_ref[k, 0] = mean[:, :half]
        o_ref[k, 1] = mean[:, half:]
        return carry

    lax.fori_loop(0, o_ref.shape[0], finish, 0, unroll=5)

def swapped(block, axis, bit):
    route = [(i, i ^ bit) for i in range(lax.axis_size(axis))]
    return lax.ppermute(block, axis, route)

def fast_device(micrograph, box_tops, box_live, box_class, box_shift):
    n_rows = lax.axis_size("rows")
    n_half = lax.axis_size("half")
    everyone = ("rows", "half")
    total = n_rows * n_half
    height, quarter = micrograph.shape
    width = quarter * n_half
    row_index = lax.axis_index("rows")
    half_index = lax.axis_index("half")
    kept = POINTS // n_half
    span = height // POINTS
    slab = quarter // n_rows
    slots = box_tops.shape[2]
    shape = jax.ShapeDtypeStruct

    below = passed_along(micrograph[:BOX], "rows", -1)
    micrograph2 = swapped(micrograph, "half", 1)

    points = np.arange(BOX)
    cos_box, sin_box = waves(points, points, BOX)

    def table(values):
        return pltpu.with_memory_space_constraint(jnp.asarray(values), pltpu.HBM)

    first = np.stack(halves(np.concatenate([cos_box, -sin_box], axis=1)))
    tc, ts = waves(np.arange(POINTS), points, width)
    mc, ms = waves(np.arange(POINTS), BOX - points, width)
    turns = np.stack([tc, ts]).astype(np.float32)[:, :, None]
    turns_both = (np.stack([tc, ts, mc, ms]) / width).astype(np.float32)[:, :, None]

    def fetched(*tables):
        return [pltpu.VMEM(t.shape, t.dtype) for t in tables] + [pltpu.SemaphoreType.DMA((len(tables),))]

    ready = call(
        functools.partial(prepare_kernel, n_half),
        shape((n_half, POINTS, quarter // POINTS, height // n_half), bf16),
        [micrograph], [VMEM],
        flops=2 * height * quarter * (height + quarter),
    )
    ready = lax.all_to_all(ready, "half", 0, 0, tiled=True)
    below2 = swapped(below, "half", 1)
    mixed = call(
        functools.partial(rows_kernel, n_rows, n_half),
        shape((total, kept, span, slab), bf16),
        [ready, table(first), table(turns)], [VMEM, HBM, HBM],
        scratch=[pltpu.VMEM((POINTS, height // n_half, BOX), f32)] * 2
        + [pltpu.VMEM((POINTS // GROUP, GROUP * height // n_half, BOX), bf16)] + fetched(first, turns),
        flops=4 * height * quarter * 2 * BOX,
    )
    mixed = lax.all_to_all(mixed, everyone, 0, 0, tiled=True)

    core = half_index % 2
    corner = jnp.stack([row_index * height, (half_index - core) * quarter])
    band_tops = box_tops[row_index]
    at = jnp.stack([band_tops[half_index], band_tops[half_index ^ 2]]) - corner
    at = jnp.concatenate([at.reshape(-1), core.reshape(1)])
    pieces, sent = call(
        pieces_kernel,
        (shape((slots, BOX, BOX), bf16),) * 2,
        [at, micrograph, below, micrograph2, below2], [SMEM] + [VMEM] * 4,
        scratch=[pltpu.VMEM((2, height + BOX, quarter), bf16)],
        flops=20 * slots * BOX * BOX,
    )
    across = swapped(sent, "half", 2)
    part = BOX // n_half

    def by_part(a, b):
        a = a.reshape(-1, n_half, 1, part)
        b = b.reshape(-1, n_half, 1, part)
        return np.concatenate([a, b], axis=2).reshape(-1, 2 * BOX)

    plain = by_part(cos_box, -sin_box)
    crossed = by_part(-sin_box, -cos_box)
    inner = np.stack(halves(np.concatenate([plain, crossed], axis=1) / BOX))
    outer = np.stack(halves(np.concatenate([cos_box, sin_box], axis=1)))
    my_tops = box_tops[row_index, half_index]
    rolls = jnp.mod(box_shift.reshape(slots, 2) - my_tops, BOX).reshape(-1)
    n_planes = n_rows // 2
    members = total // n_planes
    plane = row_index // 2
    member = (row_index % 2) * n_half + half_index
    spot = jnp.stack([plane, row_index % 2, half_index])
    spectra = call(
        functools.partial(spectra_kernel, n_planes, n_half),
        (shape((n_planes, slots, BOX // n_rows, 2 * part), bf16),) * members,
        [jnp.concatenate([rolls, spot]), pieces, across, table(inner), table(outer)],
        [SMEM, VMEM, VMEM, HBM, HBM],
        scratch=[pltpu.VMEM(t.shape, t.dtype) for t in (inner, outer)] + fetched(inner, outer),
        flops=slots * BOX * BOX * 4 * BOX * 10,
    )
    sides = [spectra[0]]
    for m in range(1, members):
        route = [(d, d - d % members + (d % members ^ m)) for d in range(total)]
        sides.append(lax.ppermute(spectra[m], everyone, route))

    def across_planes(blocks):
        count = len(blocks)
        gathered = call(
            functools.partial(gather_kernel, count),
            (shape((count * slots, BOX // n_rows, 2 * part), bf16),) * n_planes,
            blocks, [VMEM] * count,
            flops=count * slots * BOX * BOX,
        )
        arrived = [gathered[0]]
        for k in range(1, n_planes):
            route = [(d, (d + k * members) % total) for d in range(total)]
            arrived.append(lax.ppermute(gathered[k], everyone, route))
        return arrived

    early = members // 2
    arrived = across_planes(sides[:early]) + across_planes(sides[early:])

    def source_order(values):
        values = values.reshape(n_planes, members, slots)
        ids = jnp.arange(max(n_planes, members), dtype=jnp.int32)
        values = values[jnp.mod(plane - ids[:n_planes], n_planes)]
        values = values[:, member ^ ids[:members]].reshape(n_planes, members // early, early, slots)
        return jnp.transpose(values, (1, 0, 2, 3)).reshape(-1)

    half = slab // 2
    place = half_index * n_rows + row_index
    own, far, edge = call(
        functools.partial(columns_kernel, n_rows, n_half),
        (shape((half, width), f32), shape((half, width), bf16), shape((width // LANES, LANES), f32)),
        [place.reshape(1), mixed, table(first), table(turns_both)], [SMEM, VMEM, HBM, HBM],
        scratch=[pltpu.VMEM((POINTS, half, BOX), f32)] * 4
        + [pltpu.VMEM((half, width), f32), pltpu.VMEM((4, 8, width), f32)]
        + [pltpu.VMEM((POINTS // GROUP, GROUP * slab, BOX), bf16)]
        + fetched(first, turns_both),
        flops=8 * slab * width * 2 * BOX,
    )
    far = lax.ppermute(far, everyone, [(d, total - 1 - d) for d in range(total)])
    seats = [(p % n_rows) * n_half + p // n_rows for p in range(total)]
    route = [(p, total - p) for p in range(1, total // 2)] + [(0, total // 2)]
    edge = lax.ppermute(edge, everyone, [(seats[a], seats[b]) for a, b in route])
    power = call(
        power_kernel,
        shape((slab, width), f32),
        [(2 * place >= total).astype(jnp.int32).reshape(1), own, far, edge], [SMEM] + [VMEM] * 3,
        flops=slab * width,
    )[None]
    labels, lives = box_class.reshape(-1), box_live.reshape(-1)
    matches = labels[None, :] == jnp.arange(CLASSES, dtype=jnp.int32)[:, None]
    counts = jnp.sum(jnp.where(matches, lives[None, :], 0), axis=1)
    divisor = jnp.maximum(counts, 1).astype(f32)
    labels_here, lives_here = source_order(box_class), source_order(box_live)
    class_means = call(
        means_kernel,
        shape((CLASSES, 2, BOX // n_rows, part), f32),
        [labels_here, lives_here, divisor, *arrived], [SMEM] * 3 + [VMEM] * len(arrived),
        scratch=[pltpu.VMEM((CLASSES, BOX // n_rows, 2 * part), f32)] * SUMS,
        flops=4 * total * slots * BOX * BOX,
    )
    return (power, class_means)

def fits(mesh, micrograph):
    height, quarter = micrograph.shape
    n_rows, n_half = mesh.shape["rows"], mesh.shape["half"]
    return (
        height * n_rows == POINTS * BOX
        and quarter * n_half == POINTS * BOX
        and n_half == 4
        and height % BOX == 0
        and quarter % BOX == 0
        and height // n_half == LANES
        and quarter // n_rows == LANES
        and BOX // n_rows % 16 == 0
        and 2 * BOX // n_half == LANES
        and n_rows == 8
    )

def solution(mesh):
    in_specs = (P("rows", "half"), P(), P(), P(), P("rows", "half", None, None))
    out_specs = (P("half", "rows", None), P(None, None, "rows", "half"))

    def per_device(micrograph, *boxes):
        device = fast_device if fits(mesh, micrograph) else general_device
        return device(micrograph, *boxes)

    return jax.shard_map(
        per_device, mesh=mesh, in_specs=in_specs, out_specs=out_specs, check_vma=False
    )
```

```python
import functools

import numpy as np

import jax
import jax.numpy as jnp
from jax import lax
from jax.experimental import pallas as pl
from jax.experimental.pallas import tpu as pltpu
from jax.sharding import PartitionSpec as P


BOX = 256
CLASSES = 50
RADIX = 64
LANES = 128
POINTS = 16

highest = lax.Precision.HIGHEST


def passed_along(block, axis, distance):
    devices = range(lax.axis_size(axis))
    route = [(i - distance, i) for i in devices if i - distance in devices]
    return lax.ppermute(block, axis, route)


def phases(left_index, right_index, length):
    rotations = jnp.mod(left_index[:, None] * right_index[None, :], length)
    angles = 2.0 * jnp.pi / length * rotations.astype(jnp.float32)
    return (jnp.cos(angles), jnp.sin(angles))


def product(pattern, left_side, matrix):
    return jnp.einsum(pattern, left_side, matrix, precision=highest)


def four_step(real_part, imag_part, first_index, how_many, rows_last):
    height = real_part.shape[0]
    length = real_part.shape[1]
    outer_size = RADIX
    inner_size = length // outer_size
    real_part = real_part.reshape(height, outer_size, inner_size)
    spread = jnp.arange(outer_size, dtype=jnp.int32)
    across = jnp.arange(inner_size, dtype=jnp.int32)
    cos_one, sin_one = phases(spread, spread, outer_size)
    section_real = product("mab,ka->mkb", real_part, cos_one)
    section_imag = -product("mab,ka->mkb", real_part, sin_one)
    if imag_part is not None:
        imag_part = imag_part.reshape(height, outer_size, inner_size)
        section_real = section_real + product("mab,ka->mkb", imag_part, sin_one)
        section_imag = section_imag + product("mab,ka->mkb", imag_part, cos_one)
    twist_cos, twist_sin = phases(spread, across, length)
    turned_real = section_real * twist_cos + section_imag * twist_sin
    turned_imag = section_imag * twist_cos - section_real * twist_sin
    wanted = first_index + jnp.arange(how_many, dtype=jnp.int32)
    cos_two, sin_two = phases(wanted, across, inner_size)
    pattern = "mkb,tb->tkm" if rows_last else "mkb,tb->mtk"
    out_real = product(pattern, turned_real, cos_two) + product(pattern, turned_imag, sin_two)
    out_imag = product(pattern, turned_imag, cos_two) - product(pattern, turned_real, sin_two)
    return (out_real, out_imag)


def general_device(micrograph, box_tops, box_live, box_class, box_shift):
    row_index = lax.axis_index("rows")
    half_index = lax.axis_index("half")
    band_rows = lax.all_gather(micrograph, "half", axis=1, tiled=True)
    height = band_rows.shape[0]
    full_width = band_rows.shape[1]
    quarter = full_width // lax.axis_size("half")
    per_block = quarter // RADIX
    image_rows = band_rows.astype(jnp.float32)
    part_real, part_imag = four_step(image_rows, None, half_index * per_block, per_block, True)
    partial_value = jnp.stack(
        [part_real.reshape(quarter, height), part_imag.reshape(quarter, height)]
    )
    columns = lax.all_to_all(partial_value, "rows", split_axis=1, concat_axis=2, tiled=True)
    column_count = columns.shape[1]
    freq_real, freq_imag = four_step(columns[0], columns[1], 0, full_width // RADIX, False)
    power_out = (freq_real * freq_real + freq_imag * freq_imag).reshape(1, column_count, full_width)
    power_out = power_out / (full_width * full_width)
    local_tops = box_tops[row_index, half_index]
    start_rows = local_tops[:, 0] - row_index * height
    start_cols = local_tops[:, 1]
    reach_bands = (BOX + height - 2) // height

    def cut_columns(source, corner):
        return lax.dynamic_slice_in_dim(source, corner, BOX, 1)

    pieces = [jax.vmap(cut_columns, (None, 0))(band_rows, start_cols)]
    for offset in range(1, reach_bands + 1):
        target = jnp.maximum(row_index - offset, 0)
        their_cols = box_tops[target, half_index][:, 1]
        outgoing = jax.vmap(cut_columns, (None, 0))(band_rows, their_cols)
        pieces.append(passed_along(outgoing, "rows", -offset))
    windows = jnp.concatenate(pieces, axis=1)
    particle_boxes = jax.vmap(
        lambda window, corner: lax.dynamic_slice_in_dim(window, corner, BOX, 0)
    )(windows, start_rows)
    frequency = jnp.arange(BOX, dtype=jnp.int32)
    cos_box, sin_box = phases(frequency, frequency, BOX)
    local_offsets = box_shift.reshape(-1, 2)

    def spectrum(member):
        particle, offsets_pair = member
        values = particle.astype(jnp.float32)
        inner_real = jnp.dot(values, cos_box, precision=highest)
        inner_imag = -jnp.dot(values, sin_box, precision=highest)
        outer_real = (
            jnp.dot(cos_box, inner_real, precision=highest)
            + jnp.dot(sin_box, inner_imag, precision=highest)
        ) / BOX
        outer_imag = (
            jnp.dot(cos_box, inner_imag, precision=highest)
            - jnp.dot(sin_box, inner_real, precision=highest)
        ) / BOX
        rotations = jnp.mod(
            frequency[:, None] * offsets_pair[0] + frequency[None, :] * offsets_pair[1], BOX
        )
        angles = 2.0 * jnp.pi / BOX * rotations.astype(jnp.float32)
        ramp_cos = jnp.cos(angles)
        ramp_sin = jnp.sin(angles)
        shifted_real = outer_real * ramp_cos + outer_imag * ramp_sin
        shifted_imag = outer_imag * ramp_cos - outer_real * ramp_sin
        return jnp.stack([shifted_real, shifted_imag]).astype(jnp.bfloat16)

    spectra = lax.map(spectrum, (particle_boxes, local_offsets))
    classes_all = jnp.arange(CLASSES, dtype=jnp.int32)
    all_labels = box_class.reshape(-1)
    all_live = box_live.reshape(-1)
    counts = jnp.sum(
        (all_labels[None, :] == classes_all[:, None]).astype(jnp.int32) * all_live[None, :], axis=1
    )
    arrived = lax.all_to_all(spectra, "rows", split_axis=2, concat_axis=0, tiled=True)
    chosen_labels = box_class[:, half_index].reshape(-1)
    chosen_live = box_live[:, half_index].reshape(-1)
    weights = (
        (chosen_labels[None, :] == classes_all[:, None]).astype(jnp.int32) * chosen_live[None, :]
    ).astype(jnp.bfloat16)
    flat_spectra = arrived.reshape(arrived.shape[0], -1)
    partial_sums = jnp.dot(weights, flat_spectra, preferred_element_type=jnp.float32)
    partial_sums = partial_sums.reshape((CLASSES,) + arrived.shape[1:])
    class_sums = lax.psum_scatter(partial_sums, "half", scatter_dimension=3, tiled=True)
    divisor = jnp.maximum(counts, 1).astype(jnp.float32)
    class_means = class_sums / divisor[:, None, None, None]
    return (power_out, class_means)


GROUP = 4
SUMS = 4
f32 = jnp.float32
bf16 = jnp.bfloat16
VMEM = pl.BlockSpec(memory_space=pltpu.VMEM)
SMEM = pl.BlockSpec(memory_space=pltpu.SMEM)
HBM = pl.BlockSpec(memory_space=pltpu.HBM)

def call(kernel, out, operands, specs, scratch=(), flops=0):
    made = out if isinstance(out, tuple) else (out,)
    moved = sum(a.size * a.dtype.itemsize for a in (*operands, *made))
    return pl.pallas_call(
        kernel,
        out_shape=out,
        in_specs=specs,
        out_specs=(VMEM,) * len(out) if isinstance(out, tuple) else VMEM,
        scratch_shapes=list(scratch),
        compiler_params=pltpu.CompilerParams(vmem_limit_bytes=48 * 1024 * 1024),
        cost_estimate=pl.CostEstimate(flops=flops, bytes_accessed=moved, transcendentals=0),
    )(*operands)

def halves(table):
    high = table.astype(bf16)
    low = (table - high.astype(np.float64)).astype(bf16)
    return high, low

def waves(left, right, length):
    angles = 2.0 * np.pi / length * np.mod(np.outer(left, right), length)
    return np.cos(angles), np.sin(angles)

def dft4(re, im):
    sr, si = re[0] + re[2], im[0] + im[2]
    dr, di = re[0] - re[2], im[0] - im[2]
    tr, ti = re[1] + re[3], im[1] + im[3]
    er, ei = re[1] - re[3], im[1] - im[3]
    return [sr + tr, dr + ei, sr - tr, dr - ei], [si + ti, di - er, si - ti, di + er]

def turn(re, im, step):
    step = step % POINTS
    if step == 0:
        return re, im
    if step == POINTS // 4:
        return im, -re
    c = float(np.cos(2.0 * np.pi * step / POINTS))
    s = float(np.sin(2.0 * np.pi * step / POINTS))
    if step == POINTS // 8:
        return (re + im) * c, (im - re) * c
    if step == 3 * POINTS // 8:
        return (im - re) * s, (re + im) * -s
    return re * c + im * s, im * c - re * s

def dft16(re, im):
    mid_re = [[None] * 4 for _ in range(4)]
    mid_im = [[None] * 4 for _ in range(4)]
    for n in range(4):
        yr, yi = dft4([re[4 * p + n] for p in range(4)], [im[4 * p + n] for p in range(4)])
        for k in range(4):
            mid_re[k][n], mid_im[k][n] = turn(yr[k], yi[k], n * k)
    out_re, out_im = [None] * POINTS, [None] * POINTS
    for k in range(4):
        yr, yi = dft4(mid_re[k], mid_im[k])
        for m in range(4):
            out_re[k + 4 * m], out_im[k + 4 * m] = yr[m], yi[m]
    return out_re, out_im

def fetch(*pairs):
    copies = [pltpu.make_async_copy(source, target, sem) for source, target, sem in pairs]
    for copy in copies:
        copy.start()
    return copies

def dot(a, b):
    return jnp.dot(a, b, preferred_element_type=f32)

def one_hot(size, wanted):
    place = lax.broadcasted_iota(jnp.int32, (size, size), 0)
    source = lax.broadcasted_iota(jnp.int32, (size, size), 1)
    return jnp.where(source == wanted(place), 1.0, 0.0).astype(bf16)

def prepare_kernel(n_half, x_ref, y_ref):
    height, quarter = x_ref.shape
    each = BOX // POINTS
    share = height // n_half
    rows_each = height // POINTS
    pick_rows = one_hot(height, lambda p: (p % rows_each) * POINTS + p // rows_each)
    pick_cols = one_hot(BOX, lambda p: (p % each) * POINTS + p // each)
    for k in range(quarter // BOX):
        ordered = dot(pick_rows, x_ref[:, k * BOX:(k + 1) * BOX]).astype(bf16)
        turned = lax.dot_general(
            pick_cols, ordered, (((1,), (1,)), ((), ())), preferred_element_type=f32
        ).astype(bf16)
        for j in range(n_half):
            for c in range(POINTS):
                y_ref[j, c, k * each:(k + 1) * each] = (
                    turned[c * each:(c + 1) * each, j * share:(j + 1) * share]
                )

def rows_kernel(n_rows, n_half, y_ref, w_hbm, t_hbm, z_ref, re_ref, im_ref, turned_ref, w_ref, t_ref, sems):
    copies = fetch((w_hbm, w_ref, sems.at[0]), (t_hbm, t_ref, sems.at[1]))
    share = y_ref.shape[3]
    span = z_ref.shape[2]
    half = LANES // 2
    lane = lax.broadcasted_iota(jnp.int32, (16, LANES), 1)

    def turn_blocks(g, carry):
        blocks = [
            jnp.concatenate([y_ref[j, g * GROUP + k] for j in range(n_half)], axis=0)
            for k in range(GROUP)
        ]
        turned_ref[g] = jnp.concatenate(blocks, axis=1).T
        return carry

    lax.fori_loop(0, POINTS // GROUP, turn_blocks, 0, unroll=2)
    for copy in copies:
        copy.wait()

    def first(g, carry):
        block = turned_ref[g]
        both = dot(block, w_ref[0]) + dot(block, w_ref[1])
        for k in range(GROUP):
            c = g * GROUP + k
            part = both[k * share:(k + 1) * share]
            re, im = part[:, :BOX], part[:, BOX:]
            tc, ts = t_ref[0, c], t_ref[1, c]
            re_ref[c] = re * tc + im * ts
            im_ref[c] = im * tc - re * ts
        return carry

    lax.fori_loop(0, POINTS // GROUP, first, 0, unroll=2)
    tiles = span // 16

    def second(t, carry):
        m = t // tiles
        at = pl.multiple_of((t % tiles) * 16, 16)
        row = pl.multiple_of(t * 16, 16)
        for h in range(BOX // LANES):
            lanes = pl.ds(h * LANES, LANES)
            re = [re_ref[c, pl.ds(row, 16), lanes] for c in range(POINTS)]
            im = [im_ref[c, pl.ds(row, 16), lanes] for c in range(POINTS)]
            re, im = dft16(re, im)
            for v in range(POINTS):
                slab = v * (BOX // LANES) + h
                to = (slab % n_rows) * n_half + slab // n_rows
                imag = pltpu.roll(im[v], half, 1)
                if 2 * slab < n_rows * n_half:
                    both = jnp.where(lane < half, re[v], imag)
                else:
                    both = jnp.where(lane < half, re[v], jnp.where(lane == half, im[v], imag))
                    both = jnp.where(lane == 0, pltpu.roll(re[v], half, 1), both)
                if slab == 0:
                    both = jnp.where(lane == half, pltpu.roll(re[POINTS // 2], half, 1), both)
                z_ref[to, m, pl.ds(at, 16), :] = both.astype(bf16)
        return carry

    lax.fori_loop(0, share // 16, second, 0, unroll=2)

def columns_kernel(n_rows, n_half, place_ref, z_ref, w_hbm, t_hbm, own_ref, far_ref, edge_ref,
                   re_ref, im_ref, mre_ref, mim_ref, mirror_ref, raw_ref, turned_ref, w_ref, t_ref, sems):
    copies = fetch((w_hbm, w_ref, sems.at[0]), (t_hbm, t_ref, sems.at[1]))
    kept = z_ref.shape[1]
    count = own_ref.shape[0]
    width = own_ref.shape[1]

    def turn_blocks(g, carry):
        blocks = []
        for k in range(GROUP):
            r = g * GROUP + k
            j, m = r // kept, r % kept
            blocks.append(
                jnp.concatenate([z_ref[i * n_half + j, m] for i in range(n_rows)], axis=0)
            )
        turned_ref[g] = jnp.concatenate(blocks, axis=1).T
        return carry

    lax.fori_loop(0, POINTS // GROUP, turn_blocks, 0, unroll=2)
    for copy in copies:
        copy.wait()

    def first(g, carry):
        block = turned_ref[g]
        product = dot(block, w_ref[0]) + dot(block, w_ref[1])
        for k in range(GROUP):
            r = g * GROUP + k
            both = product[2 * count * k:2 * count * (k + 1)]
            a, b = both[:count, :BOX], both[count:, :BOX]
            c, d = both[:count, BOX:], both[count:, BOX:]
            tc, ts = t_ref[0, r], t_ref[1, r]
            re, im = a - d, b + c
            re_ref[r] = re * tc + im * ts
            im_ref[r] = im * tc - re * ts
            tc, ts = t_ref[2, r], t_ref[3, r]
            re, im = a + d, b - c
            mre_ref[r] = re * tc + im * ts
            mim_ref[r] = im * tc - re * ts
        return carry

    lax.fori_loop(0, POINTS // GROUP, first, 0, unroll=2)

    def tile(t, raw):
        row = pl.multiple_of(t * 8, 8)
        for h in range(BOX // LANES):
            lanes = pl.ds(h * LANES, LANES)
            re = [re_ref[c, pl.ds(row, 8), lanes] for c in range(POINTS)]
            im = [im_ref[c, pl.ds(row, 8), lanes] for c in range(POINTS)]
            re, im = dft16(re, im)
            for u in range(POINTS):
                to = pl.ds(u * BOX + h * LANES, LANES)
                if raw:
                    raw_ref[0, :, to], raw_ref[1, :, to] = re[u], im[u]
                else:
                    own_ref[pl.ds(row, 8), to] = re[u] * re[u] + im[u] * im[u]
            re = [mre_ref[c, pl.ds(row, 8), lanes] for c in range(POINTS)]
            im = [mim_ref[c, pl.ds(row, 8), lanes] for c in range(POINTS)]
            re, im = dft16(re, im)
            for u in range(POINTS):
                to = pl.ds((POINTS - 1 - u) * BOX + h * LANES, LANES)
                if raw:
                    raw_ref[2, :, to], raw_ref[3, :, to] = re[u], im[u]
                else:
                    mirror_ref[pl.ds(row, 8), to] = re[u] * re[u] + im[u] * im[u]

    def second(t, carry):
        tile(t, False)
        return carry

    lax.fori_loop(0, count // 8, second, 0, unroll=2)
    tile(0, True)
    origin = place_ref[0] == 0
    for k in range(width // LANES):
        to = pl.ds(k * LANES, LANES)
        re, im, mre, mim = (raw_ref[n, 0:1, to] for n in range(4))
        even = 0.25 * ((re + mre) * (re + mre) + (im - mim) * (im - mim))
        odd = 0.25 * ((re - mre) * (re - mre) + (im + mim) * (im + mim))
        own_ref[0:1, to] = jnp.where(origin, even, own_ref[0:1, to])
        edge_ref[k:k + 1, :] = jnp.where(origin, odd, mirror_ref[0:1, to])
    place = lax.broadcasted_iota(jnp.int32, (count, count), 0)
    source = lax.broadcasted_iota(jnp.int32, (count, count), 1)
    flip = jnp.where((place + source) % count == 0, 1.0, 0.0).astype(bf16)
    for k in range(POINTS):
        to = pl.ds(k * BOX, BOX)
        far_ref[:, to] = dot(flip, mirror_ref[:, to].astype(bf16)).astype(bf16)

def power_kernel(place_ref, own_ref, far_ref, edge_ref, o_ref):
    count, width = own_ref.shape
    upper = place_ref[0] != 0
    o_ref[pl.ds(0, count), :] = own_ref[...]
    o_ref[pl.ds(count, count), :] = far_ref[...].astype(f32)
    for k in range(width // LANES):
        to = pl.ds(k * LANES, LANES)
        o_ref[0:1, to] = jnp.where(upper, edge_ref[k:k + 1, :], own_ref[0:1, to])
        o_ref[count:count + 1, to] = jnp.where(upper, own_ref[0:1, to], o_ref[count:count + 1, to])

def pieces_kernel(at_ref, x_ref, low_ref, x2_ref, low2_ref, own_ref, sent_ref, ext_ref):
    height, quarter = x_ref.shape
    tall, wide = height // BOX, quarter // BOX
    slots = own_ref.shape[0]
    chunk = 64
    mine = at_ref[4 * slots]
    ext_ref[mine, pl.ds(0, height), :] = x_ref[...]
    ext_ref[mine, pl.ds(height, BOX), :] = low_ref[...]
    ext_ref[1 - mine, pl.ds(0, height), :] = x2_ref[...]
    ext_ref[1 - mine, pl.ds(height, BOX), :] = low2_ref[...]

    def one(o_ref, first_slot, s):
        slot = first_slot + s
        top, left = at_ref[2 * slot], at_ref[2 * slot + 1]
        tile_row = jnp.clip(top >> 8, 0, tall - 1)
        tile_col = left >> 8
        row_cut, col_cut = top & (BOX - 1), left & (BOX - 1)
        here = jnp.logical_and(tile_col >= 0, tile_col < 2 * wide).astype(f32)
        after = jnp.logical_and(tile_col >= -1, tile_col < 2 * wide - 1).astype(f32)
        tile_a = jnp.clip(tile_col, 0, 2 * wide - 1)
        tile_b = jnp.clip(tile_col + 1, 0, 2 * wide - 1)
        side_a, side_b = tile_a // wide, tile_b // wide
        col_a = pl.multiple_of((tile_a % wide) * BOX, BOX)
        col_b = pl.multiple_of((tile_b % wide) * BOX, BOX)
        right = lax.broadcasted_iota(jnp.int32, (chunk, BOX), 1) >= col_cut
        rows = lax.broadcasted_iota(jnp.int32, (chunk, BOX), 0)
        for k in range(BOX // chunk):
            upper = pl.multiple_of(tile_row * BOX + k * chunk, chunk)
            lower = pl.multiple_of(tile_row * BOX + BOX + k * chunk, chunk)

            def across(first_row):
                a = ext_ref[side_a, pl.ds(first_row, chunk), pl.ds(col_a, BOX)].astype(f32) * here
                b = ext_ref[side_b, pl.ds(first_row, chunk), pl.ds(col_b, BOX)].astype(f32) * after
                return jnp.where(right, a, b)

            whole = jnp.where(rows + k * chunk >= row_cut, across(upper), across(lower))
            o_ref[s, pl.ds(k * chunk, chunk), :] = whole.astype(bf16)

    def both(s, carry):
        one(own_ref, 0, s)
        one(sent_ref, slots, s)
        return carry

    lax.fori_loop(0, slots, both, 0)

def spectra_kernel(n_planes, n_half, at_ref, p_ref, q_ref, w_hbm, c_hbm, *refs):
    members = len(refs) - 5
    o_refs, (w_ref, c_ref, w2_ref, c2_ref, sems) = refs[:members], refs[members:]
    copies = fetch((w_hbm, w_ref, sems.at[0]), (c_hbm, c_ref, sems.at[1]))
    slots = q_ref.shape[0]
    wide = 2 * BOX
    band = wide // n_half
    tall = o_refs[0].shape[2]
    beside = members // n_half
    plane, side, column = (at_ref[2 * slots + n] for n in range(3))
    for copy in copies:
        copy.wait()
    for part in range(2):
        for k in range(n_planes):
            for i in range(beside):
                first = (lax.rem(plane + k, n_planes) * beside + (side ^ i)) * tall
                rows = c_ref[part, pl.ds(pl.multiple_of(first, tall), tall), :]
                c2_ref[part, pl.ds((k * beside + i) * tall, tall), :] = rows
        for half in range(2):
            for j in range(n_half):
                first = pl.multiple_of((column ^ j) * band + half * wide, band)
                w2_ref[part, :, pl.ds(j * band + half * wide, band)] = w_ref[part, :, pl.ds(first, band)]

    def one(s, carry):
        box = p_ref[s].astype(f32) + q_ref[s].astype(f32)
        box = pltpu.roll(box, at_ref[2 * s], 0)
        box = pltpu.roll(box, at_ref[2 * s + 1], 1).astype(bf16)
        inner = dot(box, w2_ref[0]) + dot(box, w2_ref[1])
        high = inner.astype(bf16)
        low = (inner - high.astype(f32)).astype(bf16)
        high = jnp.concatenate([high[:, :wide], high[:, wide:]], axis=0)
        low = jnp.concatenate([low[:, :wide], low[:, wide:]], axis=0)
        outer = dot(c2_ref[0], high) + dot(c2_ref[0], low) + dot(c2_ref[1], high)
        outer = outer.astype(bf16)
        for k in range(n_planes):
            for i in range(beside):
                row = (k * beside + i) * tall
                for j in range(n_half):
                    o_refs[i * n_half + j][k, s] = outer[row:row + tall, j * band:(j + 1) * band]
        return carry

    lax.fori_loop(0, slots, one, 0, unroll=2)

def gather_kernel(members, *refs):
    sides, outs = refs[:members], refs[members:]
    slots = sides[0].shape[1]
    for k, out_ref in enumerate(outs):
        for m, side_ref in enumerate(sides):
            out_ref[pl.ds(m * slots, slots)] = side_ref[k]

def means_kernel(label_ref, live_ref, divisor_ref, *refs):
    count = len(refs) - 1 - SUMS
    f_refs, o_ref, sum_refs = refs[:count], refs[count], refs[count + 1:]
    here = f_refs[0].shape[0]
    half = f_refs[0].shape[2] // 2
    for sum_ref in sum_refs:
        sum_ref[...] = jnp.zeros_like(sum_ref)

    def add(g, carry):
        for n, f_ref in enumerate(f_refs):
            sum_ref = sum_refs[n % SUMS]
            k = label_ref[n * here + g]
            live = live_ref[n * here + g].astype(f32)
            sum_ref[k] = sum_ref[k] + f_ref[g].astype(f32) * live
        return carry

    lax.fori_loop(0, here, add, 0, unroll=4)

    def finish(k, carry):
        mean = sum_refs[0][k]
        for sum_ref in sum_refs[1:]:
            mean = mean + sum_ref[k]
        mean = mean / divisor_ref[k]
        o_ref[k, 0] = mean[:, :half]
        o_ref[k, 1] = mean[:, half:]
        return carry

    lax.fori_loop(0, o_ref.shape[0], finish, 0, unroll=5)

def swapped(block, axis, bit):
    route = [(i, i ^ bit) for i in range(lax.axis_size(axis))]
    return lax.ppermute(block, axis, route)

def fast_device(micrograph, box_tops, box_live, box_class, box_shift):
    n_rows = lax.axis_size("rows")
    n_half = lax.axis_size("half")
    everyone = ("rows", "half")
    total = n_rows * n_half
    height, quarter = micrograph.shape
    width = quarter * n_half
    row_index = lax.axis_index("rows")
    half_index = lax.axis_index("half")
    kept = POINTS // n_half
    span = height // POINTS
    slab = quarter // n_rows
    slots = box_tops.shape[2]
    shape = jax.ShapeDtypeStruct

    below = passed_along(micrograph[:BOX], "rows", -1)
    micrograph2 = swapped(micrograph, "half", 1)

    points = np.arange(BOX)
    cos_box, sin_box = waves(points, points, BOX)

    def table(values):
        return pltpu.with_memory_space_constraint(jnp.asarray(values), pltpu.HBM)

    first = np.stack(halves(np.concatenate([cos_box, -sin_box], axis=1)))
    tc, ts = waves(np.arange(POINTS), points, width)
    mc, ms = waves(np.arange(POINTS), BOX - points, width)
    turns = np.stack([tc, ts]).astype(np.float32)[:, :, None]
    turns_both = (np.stack([tc, ts, mc, ms]) / width).astype(np.float32)[:, :, None]

    def fetched(*tables):
        return [pltpu.VMEM(t.shape, t.dtype) for t in tables] + [pltpu.SemaphoreType.DMA((len(tables),))]

    ready = call(
        functools.partial(prepare_kernel, n_half),
        shape((n_half, POINTS, quarter // POINTS, height // n_half), bf16),
        [micrograph], [VMEM],
        flops=2 * height * quarter * (height + quarter),
    )
    ready = lax.all_to_all(ready, "half", 0, 0, tiled=True)
    below2 = swapped(below, "half", 1)
    mixed = call(
        functools.partial(rows_kernel, n_rows, n_half),
        shape((total, kept, span, slab), bf16),
        [ready, table(first), table(turns)], [VMEM, HBM, HBM],
        scratch=[pltpu.VMEM((POINTS, height // n_half, BOX), f32)] * 2
        + [pltpu.VMEM((POINTS // GROUP, GROUP * height // n_half, BOX), bf16)] + fetched(first, turns),
        flops=4 * height * quarter * 2 * BOX,
    )
    mixed = lax.all_to_all(mixed, everyone, 0, 0, tiled=True)

    core = half_index % 2
    corner = jnp.stack([row_index * height, (half_index - core) * quarter])
    band_tops = box_tops[row_index]
    at = jnp.stack([band_tops[half_index], band_tops[half_index ^ 2]]) - corner
    at = jnp.concatenate([at.reshape(-1), core.reshape(1)])
    pieces, sent = call(
        pieces_kernel,
        (shape((slots, BOX, BOX), bf16),) * 2,
        [at, micrograph, below, micrograph2, below2], [SMEM] + [VMEM] * 4,
        scratch=[pltpu.VMEM((2, height + BOX, quarter), bf16)],
        flops=20 * slots * BOX * BOX,
    )
    across = swapped(sent, "half", 2)
    part = BOX // n_half

    def by_part(a, b):
        a = a.reshape(-1, n_half, 1, part)
        b = b.reshape(-1, n_half, 1, part)
        return np.concatenate([a, b], axis=2).reshape(-1, 2 * BOX)

    plain = by_part(cos_box, -sin_box)
    crossed = by_part(-sin_box, -cos_box)
    inner = np.stack(halves(np.concatenate([plain, crossed], axis=1) / BOX))
    outer = np.stack(halves(np.concatenate([cos_box, sin_box], axis=1)))
    my_tops = box_tops[row_index, half_index]
    rolls = jnp.mod(box_shift.reshape(slots, 2) - my_tops, BOX).reshape(-1)
    n_planes = n_rows // 2
    members = total // n_planes
    plane = row_index // 2
    member = (row_index % 2) * n_half + half_index
    spot = jnp.stack([plane, row_index % 2, half_index])
    spectra = call(
        functools.partial(spectra_kernel, n_planes, n_half),
        (shape((n_planes, slots, BOX // n_rows, 2 * part), bf16),) * members,
        [jnp.concatenate([rolls, spot]), pieces, across, table(inner), table(outer)],
        [SMEM, VMEM, VMEM, HBM, HBM],
        scratch=[pltpu.VMEM(t.shape, t.dtype) for t in (inner, outer)] + fetched(inner, outer),
        flops=slots * BOX * BOX * 4 * BOX * 10,
    )
    sides = [spectra[0]]
    for m in range(1, members):
        route = [(d, d - d % members + (d % members ^ m)) for d in range(total)]
        sides.append(lax.ppermute(spectra[m], everyone, route))

    def across_planes(blocks):
        count = len(blocks)
        gathered = call(
            functools.partial(gather_kernel, count),
            (shape((count * slots, BOX // n_rows, 2 * part), bf16),) * n_planes,
            blocks, [VMEM] * count,
            flops=count * slots * BOX * BOX,
        )
        arrived = [gathered[0]]
        for k in range(1, n_planes):
            route = [(d, (d + k * members) % total) for d in range(total)]
            arrived.append(lax.ppermute(gathered[k], everyone, route))
        return arrived

    early = members // 2
    arrived = across_planes(sides[:early]) + across_planes(sides[early:])

    def source_order(values):
        values = values.reshape(n_planes, members, slots)
        ids = jnp.arange(max(n_planes, members), dtype=jnp.int32)
        values = values[jnp.mod(plane - ids[:n_planes], n_planes)]
        values = values[:, member ^ ids[:members]].reshape(n_planes, members // early, early, slots)
        return jnp.transpose(values, (1, 0, 2, 3)).reshape(-1)

    half = slab // 2
    place = half_index * n_rows + row_index
    own, far, edge = call(
        functools.partial(columns_kernel, n_rows, n_half),
        (shape((half, width), f32), shape((half, width), bf16), shape((width // LANES, LANES), f32)),
        [place.reshape(1), mixed, table(first), table(turns_both)], [SMEM, VMEM, HBM, HBM],
        scratch=[pltpu.VMEM((POINTS, half, BOX), f32)] * 4
        + [pltpu.VMEM((half, width), f32), pltpu.VMEM((4, 8, width), f32)]
        + [pltpu.VMEM((POINTS // GROUP, GROUP * slab, BOX), bf16)]
        + fetched(first, turns_both),
        flops=8 * slab * width * 2 * BOX,
    )
    far = lax.ppermute(far, everyone, [(d, total - 1 - d) for d in range(total)])
    seats = [(p % n_rows) * n_half + p // n_rows for p in range(total)]
    route = [(p, total - p) for p in range(1, total // 2)] + [(0, total // 2)]
    edge = lax.ppermute(edge, everyone, [(seats[a], seats[b]) for a, b in route])
    power = call(
        power_kernel,
        shape((slab, width), f32),
        [(2 * place >= total).astype(jnp.int32).reshape(1), own, far, edge], [SMEM] + [VMEM] * 3,
        flops=slab * width,
    )[None]
    labels, lives = box_class.reshape(-1), box_live.reshape(-1)
    matches = labels[None, :] == jnp.arange(CLASSES, dtype=jnp.int32)[:, None]
    counts = jnp.sum(jnp.where(matches, lives[None, :], 0), axis=1)
    divisor = jnp.maximum(counts, 1).astype(f32)
    labels_here, lives_here = source_order(box_class), source_order(box_live)
    class_means = call(
        means_kernel,
        shape((CLASSES, 2, BOX // n_rows, part), f32),
        [labels_here, lives_here, divisor, *arrived], [SMEM] * 3 + [VMEM] * len(arrived),
        scratch=[pltpu.VMEM((CLASSES, BOX // n_rows, 2 * part), f32)] * SUMS,
        flops=4 * total * slots * BOX * BOX,
    )
    return (power, class_means)

def fits(mesh, micrograph):
    height, quarter = micrograph.shape
    n_rows, n_half = mesh.shape["rows"], mesh.shape["half"]
    return (
        height * n_rows == POINTS * BOX
        and quarter * n_half == POINTS * BOX
        and n_half == 4
        and height % BOX == 0
        and quarter % BOX == 0
        and height // n_half == LANES
        and quarter // n_rows == LANES
        and BOX // n_rows % 16 == 0
        and 2 * BOX // n_half == LANES
        and n_rows == 8
    )

def solution(mesh):
    in_specs = (P("rows", "half"), P(), P(), P(), P("rows", "half", None, None))
    out_specs = (P("half", "rows", None), P(None, None, "rows", "half"))

    def per_device(micrograph, *boxes):
        device = fast_device if fits(mesh, micrograph) else general_device
        return device(micrograph, *boxes)

    return jax.shard_map(
        per_device, mesh=mesh, in_specs=in_specs, out_specs=out_specs, check_vma=False
    )
```
